512 devices in a mesh: tier: 64 (over x, z, core), sys: 8 (over y).
Axes of the slice: x: 4, y: 8, z: 8, core: 2. Of those that a mesh axis runs over, the one named last changes fastest.
Arguments:
- state: float32 [256, 2, 512, 512], P('tier', None, 'sys'), may hold values from -6 to 6
- slope: float32 [256, 2, 512, 512], P('tier', None, 'sys'), may hold values from -6 to 6
- counts: int32 [64], replicated, may hold values from 1 to 4, 128 in all
- links: int32 [4, 256, 96], P(None, 'tier'), may hold values from 0 to 255, as said below
- mode_site: int32 [48], replicated, may hold values from 0 to 511, as said below
- mode_coef: float32 [2, 48], replicated, may hold values from -3 to 3
- mode_rate: float32 [48], replicated, may hold values from 0.01 to 0.1
- h_bands: float32 [9, 512], replicated, may hold values from -3 to 3
Outputs:
- slope_next: float32 [256, 2, 512, 512], P('tier', None, 'sys')
- partial_sum: float32 [256, 2, 512, 512], P('tier', None, 'sys')
The draws below stay inside these ranges and needn't reach their ends.
Inputs may be any that keep to these rules, and one draw needn't show every extreme that they name: Index d of tier holds counts[d] live auxiliary operators, in its first slots; the counts sum to 128. links[0] is a global slot (index of tier times 4 plus the slot), links[1] a mode below 48, links[2] is 0 or 1, links[3] is 1 or 2. Each slot has exactly one link with direction 0 and one with direction 1 for every mode. Of the 384 links of the slots of one index of tier, exactly 6 name slots of each index of tier; of the links whose mode k has k // 6 equal to one row block's number, at most 2 name slots of one index of tier, and in every row block some index of tier is named by exactly 2 of them. `mode_site`: mode k's site lies in row block k // 6, that is in rows (k // 6) * 64 to (k // 6) * 64 + 63; the sites are distinct.
All inputs are finite; a program needn't handle non-finite values.
Results may differ from the reference program's by a relative error of at most 0.0003.
Values sent between devices are 32-bit elements; how exact they have to be, the bound alone decides.
No kernel may reach another device: no remote copies, remote signals or barrier semaphores. Data moves between devices by JAX's collectives and lax.ppermute only.
A program may use at most 64 MiB of HBM per device.

```python
import math
import jax
import jax.numpy as jnp
import numpy as np
from jax import lax

LEVELS = 512
BAND = 8
MODES_BLK = 6
SLOTS = 4
SLOTS_ALL = 256
ADOS = 128
MODES = 48
LINKS = 96
ROWS_DEV = 64
N_TIER = 64
N_SYS = 8


def draw_links(key, part):
    per_block = SLOTS * 2 * MODES_BLK

    def one_device(device_key):
        key_holder, key_order, key_slot, key_level = jax.random.split(device_key, 4)
        holders = jax.random.permutation(key_holder, N_TIER).astype(jnp.int32)
        order = jax.vmap(lambda block_key: jax.random.permutation(block_key, per_block))(jax.random.split(key_order, N_SYS)).astype(jnp.int32)
        base = jnp.arange(N_SYS, dtype=jnp.int32)[:, None] * per_block + order
        holder = holders[base // 2 % N_TIER]
        within = jnp.arange(per_block, dtype=jnp.int32)
        target_slot = jax.random.randint(key_slot, (N_SYS, per_block), 0, SLOTS, dtype=jnp.int32)
        mode_pick = jnp.arange(N_SYS, dtype=jnp.int32)[:, None] * MODES_BLK + (within // 2 % MODES_BLK)[None, :]
        link_kind = jnp.broadcast_to((within % 2)[None, :], (N_SYS, per_block))
        link_level = jax.random.randint(key_level, (N_SYS, per_block), 1, 3, dtype=jnp.int32)
        stacked = jnp.stack([holder * SLOTS + target_slot, mode_pick, link_kind, link_level])
        stacked = stacked.reshape(4, N_SYS, SLOTS, 2 * MODES_BLK)
        return jnp.transpose(stacked, (0, 2, 1, 3)).reshape(4, SLOTS, LINKS)
    devices = jax.vmap(one_device)(jax.random.split(jax.random.fold_in(key, 11), N_TIER))
    return jnp.transpose(devices, (1, 0, 2, 3)).reshape(4, SLOTS_ALL, LINKS).astype(jnp.int32)


def draw_mode_site(key, part):

    def one_block(block_key):
        return jax.random.permutation(block_key, ROWS_DEV)[:MODES_BLK].astype(jnp.int32)
    chosen = jax.vmap(one_block)(jax.random.split(jax.random.fold_in(key, 23), N_SYS))
    offsets = ROWS_DEV * jnp.arange(N_SYS, dtype=jnp.int32)[:, None]
    return (chosen + offsets).reshape(MODES).astype(jnp.int32)


def level_of(own_key, shape, shards, least, top_value):
    def one(axis_at, parts):
        steps = jax.random.uniform(jax.random.fold_in(jax.random.fold_in(own_key, 6), axis_at), (parts,), jnp.float32, least / len(shards), top_value / len(shards))
        return jnp.repeat(jnp.exp(steps), shape[axis_at] // parts).reshape((-1,) + (1,) * (len(shape) - axis_at - 1))

    level = one(*shards[0])
    for cut in shards[1:]:
        level = level * one(*cut)
    return level


def length_profile(count, total, bound, lean):
    loads = [(1 << 20) // math.isqrt(grade ** lean) + 1 for grade in range(2, count + 1)]
    spare, given = total - bound - (count - 1), [1] * (count - 1)
    while spare > 0:
        movable = [i for i in range(count - 1) if given[i] < bound]
        whole, remaining = sum([loads[i] for i in movable]), spare
        for i in movable:
            more = min(bound - given[i], max(1, remaining * loads[i] // whole), spare)
            given[i] = given[i] + more
            spare = spare - more
    return np.array([bound] + given)


def ragged_sizes(stream_key, count, total, reach, lean):
    if count == 2:
        one = jax.random.randint(stream_key, (), max(1, total - reach), min(reach, total - 1) + 1)
        return jnp.stack([one, total - one])
    lengths = jnp.asarray(length_profile(count, total, reach, lean), jnp.int32)
    twos = (count - 1) // 2
    source_of, sink = lengths[1:1 + 2 * twos:2], lengths[2:2 + 2 * twos:2]
    slack = jnp.minimum(source_of - 1, reach - sink)
    shifted = jax.random.randint(jax.random.fold_in(stream_key, 1), (twos,), 0, 1 << 20) % (slack + 1)
    lengths = lengths.at[1:1 + 2 * twos:2].set(source_of - shifted).at[2:2 + 2 * twos:2].set(sink + shifted)
    return lengths[jax.random.permutation(jax.random.fold_in(stream_key, 2), count)]


def centred(rng, extent, width, most, shards=(), kind=jnp.bfloat16):
    values = width * jax.random.normal(rng, extent, jnp.float32)
    if shards:
        values = values * level_of(rng, extent, shards, -0.22, 0.18)
    return jnp.clip(values, -most, most).astype(kind)


def setup_inputs(seed: int = 0) -> dict:
    seeds = jax.random.split(jax.random.key(seed), 9)
    state = centred(seeds[0], (SLOTS_ALL, 2, LEVELS, LEVELS), 1.0, 6.0, ((0, 64), (2, 8)), jnp.float32)
    slope = centred(seeds[1], (SLOTS_ALL, 2, LEVELS, LEVELS), 1.0, 6.0, ((0, 64), (2, 8)), jnp.float32)
    counts = ragged_sizes(seeds[2], N_TIER, ADOS, SLOTS, 2).astype(jnp.int32)
    links = draw_links(jax.random.fold_in(seeds[8], 71), 0)
    mode_site = draw_mode_site(jax.random.fold_in(seeds[8], 71), 0)
    mode_coef = centred(seeds[5], (2, MODES), 0.5, 3.0, (), jnp.float32)
    mode_rate = jnp.clip(jnp.exp(jax.random.uniform(seeds[6], (MODES,), jnp.float32, math.log(0.01), math.log(0.1))), 0.01, 0.1)
    h_bands = centred(seeds[7], (BAND + 1, LEVELS), 0.5, 3.0, (), jnp.float32)
    return {"state": state, "slope": slope, "counts": counts, "links": links, "mode_site": mode_site, "mode_coef": mode_coef, "mode_rate": mode_rate, "h_bands": h_bands}


step_size = 0.05


def shifted_band(h_bands):
    band_width = h_bands.shape[0] - 1
    length = h_bands.shape[1]
    padded = jnp.pad(h_bands, ((0, 0), (band_width, 0)))
    return jnp.stack([padded[offset, band_width - offset:band_width - offset + length] for offset in range(band_width + 1)])


def band_rows(padded, upper_band, lower_band, band_width):
    length = upper_band.shape[1]
    summed = upper_band[0][:, None] * padded[..., band_width:band_width + length, :]
    for offset in range(1, band_width + 1):
        summed = summed + upper_band[offset][:, None] * padded[..., band_width + offset:band_width + offset + length, :]
        summed = summed + lower_band[offset][:, None] * padded[..., band_width - offset:band_width - offset + length, :]
    return summed


def band_cols(field, upper_band, lower_band, band_width):
    length = field.shape[-1]
    padded = jnp.pad(field, ((0, 0),) * (field.ndim - 1) + ((band_width, band_width),))
    summed = upper_band[0] * field
    for offset in range(1, band_width + 1):
        summed = summed + upper_band[offset] * padded[..., band_width + offset:band_width + offset + length]
        summed = summed + lower_band[offset] * padded[..., band_width - offset:band_width - offset + length]
    return summed


def reference(state, slope, counts, links, mode_site, mode_coef, mode_rate, h_bands):
    midpoint = state + (0.5 * step_size) * slope
    every_slot = jnp.arange(SLOTS_ALL, dtype=jnp.int32)
    live = (every_slot % SLOTS < counts[every_slot // SLOTS]).astype(jnp.float32)
    lower_band = shifted_band(h_bands)

    def derive(carry, inputs):
        field, link_set = inputs
        neighbour = link_set[0]
        link_mode = link_set[1]
        link_kind = link_set[2]
        link_level = link_set[3].astype(jnp.float32)
        sites = mode_site[link_mode]
        downward = link_kind == 1
        neighbour_live = live[neighbour]
        weight_re = jnp.where(downward, link_level * mode_coef[0][link_mode], 1.0) * neighbour_live
        weight_im = jnp.where(downward, link_level * mode_coef[1][link_mode], 0.0) * neighbour_live
        damping = jnp.sum(jnp.where(downward, link_level * mode_rate[link_mode], 0.0))
        column_part = midpoint[neighbour, :, :, sites]
        row_part = midpoint[neighbour, :, sites, :]
        padded = jnp.pad(field, ((0, 0), (BAND, BAND), (0, 0)))
        commuted = band_rows(padded, h_bands, lower_band, BAND) - band_cols(field, h_bands, lower_band, BAND)
        deriv_re = commuted[1] - damping * field[0]
        deriv_im = -commuted[0] - damping * field[1]
        col_re = -(weight_re[:, None] * column_part[:, 1] - weight_im[:, None] * column_part[:, 0])
        col_im = weight_re[:, None] * column_part[:, 0] + weight_im[:, None] * column_part[:, 1]
        row_re = weight_re[:, None] * row_part[:, 1] + weight_im[:, None] * row_part[:, 0]
        row_im = -(weight_re[:, None] * row_part[:, 0] - weight_im[:, None] * row_part[:, 1])
        deriv_re = deriv_re.at[:, sites].add(col_re.T)
        deriv_im = deriv_im.at[:, sites].add(col_im.T)
        deriv_re = deriv_re.at[sites, :].add(row_re)
        deriv_im = deriv_im.at[sites, :].add(row_im)
        return carry, jnp.stack([deriv_re, deriv_im])

    _, derived = lax.scan(derive, jnp.zeros((), jnp.float32), (midpoint, jnp.moveaxis(links, 1, 0)))
    slope_next = derived * live[:, None, None, None]
    partial_sum = (state + (step_size / 6.0) * slope + (step_size / 3.0) * slope_next) * live[:, None, None, None]
    return slope_next, partial_sum
```

```python
import functools

import jax
import jax.numpy as jnp
from jax import lax
from jax.experimental import pallas as pl
from jax.experimental.pallas import tpu as pltpu
from jax.sharding import PartitionSpec as P

step_size = 0.05
LANES = 128
vmem_limit = 16 * 1024 * 1024
BF16 = jnp.bfloat16
F32 = jnp.float32
VMEM = pl.BlockSpec(memory_space=pltpu.VMEM)
SMEM = pl.BlockSpec(memory_space=pltpu.SMEM)
ANY = pl.BlockSpec(memory_space=pl.ANY)


def iota(shape, dim):
    return lax.broadcasted_iota(jnp.int32, shape, dim)


def round_up(value, multiple):
    return -(-value // multiple) * multiple


def dot_nn(a, b):
    return lax.dot_general(a, b, (((1,), (0,)), ((), ())), preferred_element_type=F32)


def dot_nt(a, b):
    return lax.dot_general(a, b, (((1,), (1,)), ((), ())), preferred_element_type=F32)


def dot_tn(a, b):
    return lax.dot_general(a, b, (((0,), (0,)), ((), ())), preferred_element_type=F32)


def thirds(x):
    first = x.astype(BF16)
    rest = x - first.astype(F32)
    second = rest.astype(BF16)
    third = (rest - second.astype(F32)).astype(BF16)
    return first, second, third


def picked(chooser, values):
    first, second, third = thirds(values)
    return dot_nn(chooser, first) + (dot_nn(chooser, second) + dot_nn(chooser, third))


def as_bf16(mask):
    return jnp.where(mask, 1.0, 0.0).astype(BF16)


def as_column(row, size):
    diagonal = iota((size, size), 0) == iota((size, size), 1)
    return jnp.sum(jnp.where(diagonal, row, jnp.zeros((), row.dtype)), axis=1, keepdims=True)


class Sizes:
    def __init__(self, state, links, h_bands, tiers, parts):
        self.slots = state.shape[0]
        self.rows = state.shape[2]
        self.levels = state.shape[3]
        self.band = h_bands.shape[0] - 1
        self.per_slot = links.shape[2]
        self.tiers = tiers
        self.parts = parts
        self.modes = self.per_slot // 2
        self.block_modes = self.modes // parts
        total = self.slots * self.per_slot
        self.cap = total // tiers
        self.row_cap = 2 * ((self.slots * self.block_modes + tiers - 1) // tiers)
        self.lane_tiles = 2 * self.levels // LANES
        self.message = self.cap + self.row_cap * self.lane_tiles
        self.ask = round_up(2 * self.cap, 16)
        self.shift = self.slots.bit_length() - 1
        self.row_pad = round_up(self.slots * self.block_modes, 16)
        self.group = round_up(self.block_modes, 8)


def holders_of(z, links_ref, g):
    neighbour = links_ref[0, g : g + 1, :]
    holder = lax.shift_right_logical(neighbour, z.shift)
    target = lax.bitwise_and(neighbour, z.slots - 1)
    hit = holder == iota((z.tiers, z.per_slot), 0)
    return hit, holder, target


def earlier_table(size):
    return as_bf16(iota((size, size), 0) < iota((size, size), 1))


def rank_of(hit, seen, earlier):
    before = dot_nn(as_bf16(hit), earlier) + seen
    return jnp.sum(jnp.where(hit, before, 0.0), axis=0, keepdims=True).astype(jnp.int32)


def ask_kernel(z, links_ref, out_ref):
    earlier = earlier_table(z.per_slot)
    ones = jnp.ones((z.per_slot, z.per_slot), BF16)
    seen = jnp.zeros((z.tiers, z.per_slot), F32)
    table = jnp.zeros((z.tiers, z.ask), F32)
    field = iota((z.ask, z.per_slot), 0)
    for g in range(z.slots):
        hit, _, target = holders_of(z, links_ref, g)
        mode = links_ref[1, g : g + 1, :]
        rank = rank_of(hit, seen, earlier)
        value = jnp.where(lax.bitwise_and(field, 1) == 0, target, mode)
        value = jnp.where(lax.shift_right_logical(field, 1) == rank, value, 0)
        chosen = as_bf16(hit)
        table = table + dot_nt(chosen, value.astype(F32).astype(BF16))
        seen = seen + dot_nn(chosen, ones)
    out_ref[...] = table.astype(jnp.int32)


def table_kernel(z, state_ref, slope_ref, sites_ref, mid_ref, low_ref, high_ref, col_ref, row_ref, rows_scr, site_scr):
    part = lax.axis_index("sys")
    span = z.slots * z.modes
    site_scr[...] = jnp.zeros_like(site_scr)
    lane = iota((1, z.levels), 1)
    for k in range(z.modes):
        site_scr[k : k + 1, :] = jnp.where(lane == sites_ref[k], 1.0, 0.0)
    at_site = site_scr[: z.modes, :].astype(BF16)
    rows_scr[...] = jnp.zeros_like(rows_scr)
    for g in range(z.slots):
        mid = state_ref[g] + (0.5 * step_size) * slope_ref[g]
        mid_ref[g] = mid
        for third, values in enumerate(thirds(mid)):
            at = third * span + g * z.modes
            col_ref[at : at + z.modes, :] = dot_nt(at_site, values).astype(BF16)
        for c in range(2):
            start = c * z.rows
            low_ref[g, c] = mid_ref[g, start : start + z.band, :]
            high_ref[g, c] = mid_ref[g, start + z.rows - z.band : start + z.rows, :]
            for k in range(z.block_modes):
                local = sites_ref[part * z.block_modes + k] - part * z.rows
                at = g * z.block_modes + k
                rows_scr[at : at + 1, c * z.levels : (c + 1) * z.levels] = mid_ref[
                    g, pl.ds(start + local, 1), :
                ]
    for third, values in enumerate(thirds(rows_scr[...])):
        row_ref[third * z.row_pad : (third + 1) * z.row_pad, :] = values


def answer_kernel(z, ask_ref, col_ref, row_ref, out_ref):
    part = lax.axis_index("sys")
    span = z.slots * z.modes
    low = part * z.block_modes
    asked = ask_ref[...]
    columns = []
    row_at = [jnp.full((z.tiers, 1), -1, jnp.int32) for _ in range(z.row_cap)]
    used = jnp.zeros((z.tiers, 1), jnp.int32)
    for p in range(z.cap):
        target = asked[:, 2 * p : 2 * p + 1]
        mode = asked[:, 2 * p + 1 : 2 * p + 2]
        columns.append(as_bf16(target * z.modes + mode == iota((z.tiers, span), 1)))
        inside = jnp.logical_and(mode >= low, mode < low + z.block_modes)
        where_row = target * z.block_modes + (mode - low)
        for j in range(z.row_cap):
            take = jnp.logical_and(inside, used == j)
            row_at[j] = jnp.where(take, where_row, row_at[j])
        used = used + jnp.where(inside, 1, 0)
    chosen = jnp.concatenate(columns, axis=0)
    found = dot_nn(chosen, col_ref[:span, :])
    for third in (1, 2):
        found = found + dot_nn(chosen, col_ref[third * span : (third + 1) * span, :])
    for p in range(z.cap):
        out_ref[pl.ds(p, z.tiers, stride=z.message), :] = found[p * z.tiers : (p + 1) * z.tiers, :]
    lanes = iota((z.tiers, z.row_pad), 1)
    chosen = jnp.concatenate([as_bf16(at == lanes) for at in row_at], axis=0)
    found = dot_nn(chosen, row_ref[: z.row_pad, :])
    for third in (1, 2):
        found = found + dot_nn(chosen, row_ref[third * z.row_pad : (third + 1) * z.row_pad, :])
    for j in range(z.row_cap):
        for t in range(z.lane_tiles):
            at = z.cap + j * z.lane_tiles + t
            out_ref[pl.ds(at, z.tiers, stride=z.message), :] = found[
                j * z.tiers : (j + 1) * z.tiers, t * LANES : (t + 1) * LANES
            ]


def choose_kernel(
    z, links_ref, counts_ref, coef_ref, rate_ref, col_ref, row_ref, col_coef_ref, row_coef_ref, damp_ref
):
    part = lax.axis_index("sys")
    low = part * z.block_modes
    earlier = earlier_table(z.per_slot)
    ones = jnp.ones((z.per_slot, z.per_slot), BF16)
    seen = jnp.zeros((z.tiers, z.per_slot), F32)
    seen_rows = jnp.zeros((z.tiers, z.per_slot), F32)
    counts = as_column(counts_ref[...], z.tiers)
    rate = as_column(rate_ref[...], z.modes)
    coefs = [as_column(coef_ref[c : c + 1, :], z.modes) for c in range(2)]
    total = z.slots * z.modes
    for g in range(z.slots):
        hit, holder, target = holders_of(z, links_ref, g)
        mode = links_ref[1, g : g + 1, :]
        kind = links_ref[2, g : g + 1, :]
        level = links_ref[3, g : g + 1, :]
        rank = rank_of(hit, seen, earlier)
        seen = seen + dot_nn(as_bf16(hit), ones)
        inside = jnp.logical_and(mode >= low, mode < low + z.block_modes)
        hit_rows = jnp.logical_and(hit, inside)
        row_rank = rank_of(hit_rows, seen_rows, earlier)
        seen_rows = seen_rows + dot_nn(as_bf16(hit_rows), ones)
        live = target < jnp.sum(jnp.where(hit, counts, 0), axis=0, keepdims=True)
        scale = jnp.where(kind == 1, level, 1)
        here = as_bf16(iota((z.cap * z.tiers, z.per_slot), 0) == rank * z.tiers + holder)
        here_row = as_bf16(
            iota((z.row_cap * z.tiers, z.per_slot), 0) == row_rank * z.tiers + holder
        )
        modes = iota((z.modes, z.per_slot), 0)
        group = iota((z.group, z.per_slot), 0)
        for way in range(2):
            wanted = jnp.logical_and(kind == way, live)
            chosen = jnp.where(jnp.logical_and(modes == mode, wanted), scale, 0)
            at = way * total + g * z.modes
            col_ref[at : at + z.modes, :] = dot_nt(
                chosen.astype(F32).astype(BF16), here
            ).astype(BF16)
            own = jnp.logical_and(group + low == mode, jnp.logical_and(inside, wanted))
            at = (way * z.slots + g) * z.group
            row_ref[at : at + z.group, :] = dot_nt(
                jnp.where(own, scale, 0).astype(F32).astype(BF16), here_row
            )
        falling = jnp.where(jnp.logical_and(modes == mode, kind == 1), level, 0).astype(F32)
        amount = jnp.sum(falling, axis=1, keepdims=True) * rate
        damp_ref[g] = jnp.broadcast_to(jnp.sum(amount, axis=0, keepdims=True), (8, LANES))
        for c in range(2):
            col_coef_ref[c, g * z.modes : (g + 1) * z.modes, :] = jnp.broadcast_to(
                coefs[c], (z.modes, LANES)
            )
            mine = jnp.where(
                iota((z.group, z.modes), 0) + low == iota((z.group, z.modes), 1),
                coef_ref[c : c + 1, :],
                0.0,
            )
            mine = jnp.where(iota((z.group, z.modes), 0) < z.block_modes, mine, 0.0)
            row_coef_ref[c, g * z.group : (g + 1) * z.group, :] = jnp.broadcast_to(
                jnp.sum(mine, axis=1, keepdims=True), (z.group, LANES)
            )


def band_kernel(z, mid_ref, low_ref, high_ref, bands_ref, damp_ref, out_ref, wide, spread, across_ref):
    part = lax.axis_index("sys")
    taps = 2 * z.band + 1
    across_ref[...] = jnp.zeros_like(across_ref)
    lane = iota((1, z.levels), 1)
    for t in range(taps):
        offset = t - z.band
        row = bands_ref[abs(offset) : abs(offset) + 1, :]
        if offset < 0:
            row = jnp.where(lane >= -offset, pltpu.roll(row, -offset, 1), 0.0)
        elif offset > 0:
            row = jnp.where(lane < z.levels - offset, row, 0.0)
        across_ref[t : t + 1, :] = row
    own = iota((z.rows, z.levels), 0) + part * z.rows == iota((z.rows, z.levels), 1)
    own = as_bf16(own)
    down = jnp.zeros((z.rows, across_ref.shape[0]), F32)
    for values in thirds(across_ref[...]):
        down = down + dot_nt(own, values)
    for t in range(taps):
        spread[t] = jnp.broadcast_to(down[:, t : t + 1], (z.rows, LANES))
    tiles = z.levels // LANES
    for g in range(z.slots):
        damp = damp_ref[g, 0:1, 0:1]
        for c in range(2):
            field = mid_ref[g, c * z.rows : (c + 1) * z.rows, :]
            wide[0 : z.band, :] = low_ref[g, c]
            wide[z.band : z.band + z.rows, :] = field
            wide[z.band + z.rows :, :] = high_ref[g, c]
            summed = across_ref[z.band : z.band + 1, :] * field
            for t in range(taps):
                if t != z.band:
                    moved = pltpu.roll(field, (z.band - t) % z.levels, 1)
                    summed = summed + across_ref[t : t + 1, :] * moved
            sides = []
            for q in range(tiles):
                lanes = slice(q * LANES, (q + 1) * LANES)
                total = spread[0] * wide[0 : z.rows, lanes]
                for t in range(1, taps):
                    total = total + spread[t] * wide[t : t + z.rows, lanes]
                sides.append(total)
            commuted = jnp.concatenate(sides, axis=1) - summed
            other = 1 - c
            sign = 1.0 if c == 1 else -1.0
            mine = mid_ref[g, other * z.rows : (other + 1) * z.rows, :]
            out_ref[g, other * z.rows : (other + 1) * z.rows, :] = sign * commuted - damp * mine


def apply_kernel(
    z, got_ref, col_ref, row_ref, col_coef_ref, row_coef_ref, deriv_ref, state_ref, slope_ref,
    counts_ref, sites_ref, next_ref, sum_ref, site_scr, next_scr, sum_scr, sem,
):
    part = lax.axis_index("sys")
    tier = lax.axis_index("tier")
    lane = iota((1, z.levels), 1)
    for k in range(z.modes):
        site_scr[k : k + 1, :] = jnp.where(lane == sites_ref[k], 1.0, 0.0)
    at_site = site_scr[: z.modes, :].astype(BF16)
    total = z.slots * z.modes
    pieces = jnp.concatenate(
        [got_ref[pl.ds(p, z.tiers, stride=z.message), :] for p in range(z.cap)], axis=0
    )
    found = picked(col_ref[...], pieces)
    up, down = found[:total], found[total:]
    sign = jnp.where(iota((1, 2 * z.rows), 1) < z.rows, -1.0, 1.0)
    cols = col_coef_ref[1] * down + sign * pltpu.roll(up + col_coef_ref[0] * down, z.rows, 1)
    pieces = jnp.concatenate(
        [
            jnp.concatenate(
                [
                    got_ref[pl.ds(z.cap + j * z.lane_tiles + t, z.tiers, stride=z.message), :]
                    for t in range(z.lane_tiles)
                ],
                axis=1,
            )
            for j in range(z.row_cap)
        ],
        axis=0,
    )
    found = picked(row_ref[...].astype(BF16), pieces)
    half = z.slots * z.group
    up, down = found[:half], found[half:]
    turned = up + row_coef_ref[0, :, 0:1] * down
    straight = row_coef_ref[1, :, 0:1] * down
    rows = (
        straight[:, : z.levels] + turned[:, z.levels :],
        straight[:, z.levels :] - turned[:, : z.levels],
    )
    for g in range(z.slots):
        mine = cols[g * z.modes : (g + 1) * z.modes, :]
        added = deriv_ref[g]
        for values in thirds(mine):
            added = added + dot_tn(values, at_site)
        next_scr[g] = added
        for k in range(z.block_modes):
            local = sites_ref[part * z.block_modes + k] - part * z.rows
            for c in range(2):
                at = pl.ds(c * z.rows + local, 1)
                next_scr[g, at, :] = (
                    next_scr[g, at, :] + rows[c][g * z.group + k : g * z.group + k + 1, :]
                )
        live = jnp.where(g < counts_ref[tier], 1.0, 0.0)
        slope_next = next_scr[g] * live
        next_scr[g] = slope_next
        sum_scr[g] = (
            state_ref[g] + (step_size / 6.0) * slope_ref[g] + (step_size / 3.0) * slope_next
        ) * live
        pltpu.make_async_copy(next_scr.at[g], next_ref.at[g], sem.at[0, g]).start()
        pltpu.make_async_copy(sum_scr.at[g], sum_ref.at[g], sem.at[1, g]).start()
    for g in range(z.slots):
        pltpu.make_async_copy(next_scr.at[g], next_ref.at[g], sem.at[0, g]).wait()
        pltpu.make_async_copy(sum_scr.at[g], sum_ref.at[g], sem.at[1, g]).wait()


def call(kernel, z, name, args, in_specs, outs, scratch=(), out_specs=None, micros=1):
    return pl.pallas_call(
        functools.partial(kernel, z),
        out_shape=outs,
        in_specs=in_specs,
        out_specs=[VMEM] * len(outs) if out_specs is None else out_specs,
        scratch_shapes=list(scratch),
        name=name,
        compiler_params=pltpu.CompilerParams(vmem_limit_bytes=vmem_limit),
        cost_estimate=pl.CostEstimate(
            flops=int(micros * 1e6), bytes_accessed=int(micros * 1e5), transcendentals=0
        ),
    )(*args)


def neighbours(low_edge, high_edge):
    count = lax.axis_size("sys")
    forward = [(i, i + 1) for i in range(count - 1)]
    backward = [(target, source) for source, target in forward]
    return lax.ppermute(high_edge, "sys", forward), lax.ppermute(low_edge, "sys", backward)


def shards(state, slope, counts, links, mode_site, mode_coef, mode_rate, h_bands):
    z = Sizes(state, links, h_bands, lax.axis_size("tier"), lax.axis_size("sys"))
    shape = jax.ShapeDtypeStruct
    flat = (z.slots, 2 * z.rows, z.levels)
    state_flat = state.reshape(flat)
    slope_flat = slope.reshape(flat)
    (ask,) = call(
        ask_kernel, z, "ask", (links,), [VMEM], [shape((z.tiers, z.ask), jnp.int32)]
    )
    asked = lax.all_to_all(
        ask.reshape(z.tiers, 1, z.ask), "tier", split_axis=0, concat_axis=0, tiled=True
    ).reshape(z.tiers, z.ask)
    edge = (z.slots, 2, z.band, z.levels)
    mid, low_edge, high_edge, col_table, row_table = call(
        table_kernel,
        z,
        "tables",
        (state_flat, slope_flat, mode_site),
        [VMEM, VMEM, SMEM],
        [
            shape(flat, F32),
            shape(edge, F32),
            shape(edge, F32),
            shape((3 * z.slots * z.modes, 2 * z.rows), BF16),
            shape((3 * z.row_pad, 2 * z.levels), BF16),
        ],
        [
            pltpu.VMEM((z.row_pad, 2 * z.levels), F32),
            pltpu.VMEM((round_up(z.modes, 16), z.levels), F32),
        ],
        micros=3,
    )
    (answer,) = call(
        answer_kernel,
        z,
        "answer",
        (asked, col_table, row_table),
        [VMEM] * 3,
        [shape((z.tiers * z.message, LANES), F32)],
    )
    got = lax.all_to_all(
        answer.reshape(z.tiers, 1, z.message * LANES),
        "tier",
        split_axis=0,
        concat_axis=0,
        tiled=True,
    ).reshape(z.tiers * z.message, LANES)
    low_edge, high_edge, answer_kept = lax.optimization_barrier((low_edge, high_edge, answer))
    above, below = neighbours(low_edge, high_edge)
    col_choice, row_choice, col_coef, row_coef, damp = call(
        choose_kernel,
        z,
        "choose",
        (links, counts[None], mode_coef, mode_rate[None]),
        [VMEM] * 4,
        [
            shape((2 * z.slots * z.modes, z.cap * z.tiers), BF16),
            shape((2 * z.slots * z.group, z.row_cap * z.tiers), F32),
            shape((2, z.slots * z.modes, LANES), F32),
            shape((2, z.slots * z.group, LANES), F32),
            shape((z.slots, 8, LANES), F32),
        ],
        micros=2,
    )
    (deriv,) = call(
        band_kernel,
        z,
        "band",
        (mid, above, below, h_bands, damp),
        [VMEM] * 5,
        [shape(flat, F32)],
        [
            pltpu.VMEM((z.rows + 2 * z.band, z.levels), F32),
            pltpu.VMEM((2 * z.band + 1, z.rows, LANES), F32),
            pltpu.VMEM((round_up(2 * z.band + 1, 16), z.levels), F32),
        ],
        micros=5,
    )
    slope_next, partial_sum = call(
        apply_kernel,
        z,
        "apply",
        (
            got, col_choice, row_choice, col_coef, row_coef, deriv, state_flat, slope_flat,
            counts, mode_site,
        ),
        [VMEM] * 8 + [SMEM] * 2,
        [shape(flat, F32), shape(flat, F32)],
        [
            pltpu.VMEM((round_up(z.modes, 8), z.levels), F32),
            pltpu.VMEM(flat, F32),
            pltpu.VMEM(flat, F32),
            pltpu.SemaphoreType.DMA((2, z.slots)),
        ],
        out_specs=[ANY, ANY],
        micros=4,
    )
    return slope_next.reshape(state.shape), partial_sum.reshape(state.shape)


def solution(mesh):
    in_specs = (
        P("tier", None, "sys", None),
        P("tier", None, "sys", None),
        P(),
        P(None, "tier", None),
        P(),
        P(),
        P(),
        P(),
    )
    out_specs = (P("tier", None, "sys", None), P("tier", None, "sys", None))
    return jax.shard_map(shards, mesh=mesh, in_specs=in_specs, out_specs=out_specs, check_vma=False)
```

```python
import functools

import jax
import jax.numpy as jnp
from jax import lax
from jax.experimental import pallas as pl
from jax.experimental.pallas import tpu as pltpu
from jax.sharding import PartitionSpec as P

step_size = 0.05
LANES = 128
mib = 1024 * 1024
vmem_limits = {"tables": 16, "band": 16, "apply": 16}
BF16 = jnp.bfloat16
F32 = jnp.float32
VMEM = pl.BlockSpec(memory_space=pltpu.VMEM)
SMEM = pl.BlockSpec(memory_space=pltpu.SMEM)
HBM = pl.BlockSpec(memory_space=pltpu.HBM)


def iota(shape, dim):
    return lax.broadcasted_iota(jnp.int32, shape, dim)


def round_up(value, multiple):
    return -(-value // multiple) * multiple


def dot_nn(a, b):
    return lax.dot_general(a, b, (((1,), (0,)), ((), ())), preferred_element_type=F32)


def dot_nt(a, b):
    return lax.dot_general(a, b, (((1,), (1,)), ((), ())), preferred_element_type=F32)


def dot_tn(a, b):
    return lax.dot_general(a, b, (((0,), (0,)), ((), ())), preferred_element_type=F32)


def thirds(x):
    first = x.astype(BF16)
    rest = x - first.astype(F32)
    second = rest.astype(BF16)
    third = (rest - second.astype(F32)).astype(BF16)
    return first, second, third


def picked(chooser, values):
    first, second, third = thirds(values)
    return dot_nn(chooser, first) + (dot_nn(chooser, second) + dot_nn(chooser, third))


def as_bf16(mask):
    return jnp.where(mask, 1.0, 0.0).astype(BF16)


def as_column(row, size):
    diagonal = iota((size, size), 0) == iota((size, size), 1)
    return jnp.sum(jnp.where(diagonal, row, jnp.zeros((), row.dtype)), axis=1, keepdims=True)


class Sizes:
    def __init__(self, state, links, h_bands, tiers, parts):
        self.slots = state.shape[0]
        self.rows = state.shape[2]
        self.levels = state.shape[3]
        self.band = h_bands.shape[0] - 1
        self.per_slot = links.shape[2]
        self.tiers = tiers
        self.parts = parts
        self.modes = self.per_slot // 2
        self.block_modes = self.modes // parts
        total = self.slots * self.per_slot
        self.cap = total // tiers
        self.row_cap = 2 * ((self.slots * self.block_modes + tiers - 1) // tiers)
        self.lane_tiles = 2 * self.levels // LANES
        self.message = self.cap + self.row_cap * self.lane_tiles
        self.ask = round_up(2 * self.cap, 16)
        self.shift = self.slots.bit_length() - 1
        self.row_pad = round_up(self.slots * self.block_modes, 16)
        self.group = round_up(self.block_modes, 8)


def holders_of(z, links_ref, g):
    neighbour = links_ref[0, g : g + 1, :]
    holder = lax.shift_right_logical(neighbour, z.shift)
    target = lax.bitwise_and(neighbour, z.slots - 1)
    hit = holder == iota((z.tiers, z.per_slot), 0)
    return hit, holder, target


def earlier_table(size):
    return as_bf16(iota((size, size), 0) < iota((size, size), 1))


def rank_of(hit, seen, earlier):
    before = dot_nn(as_bf16(hit), earlier) + seen
    return jnp.sum(jnp.where(hit, before, 0.0), axis=0, keepdims=True).astype(jnp.int32)


def ask_kernel(z, links_ref, out_ref):
    earlier = earlier_table(z.per_slot)
    ones = jnp.ones((z.per_slot, z.per_slot), BF16)
    seen = jnp.zeros((z.tiers, z.per_slot), F32)
    table = jnp.zeros((z.tiers, z.ask), F32)
    field = iota((z.ask, z.per_slot), 0)
    for g in range(z.slots):
        hit, _, target = holders_of(z, links_ref, g)
        mode = links_ref[1, g : g + 1, :]
        rank = rank_of(hit, seen, earlier)
        value = jnp.where(lax.bitwise_and(field, 1) == 0, target, mode)
        value = jnp.where(lax.shift_right_logical(field, 1) == rank, value, 0)
        chosen = as_bf16(hit)
        table = table + dot_nt(chosen, value.astype(F32).astype(BF16))
        seen = seen + dot_nn(chosen, ones)
    out_ref[...] = table.astype(jnp.int32)


def fetches(z, sources, targets, sem):
    every = []
    for g in range(z.slots):
        pair = [
            pltpu.make_async_copy(source.at[g], target.at[g], sem.at[i, g])
            for i, (source, target) in enumerate(zip(sources, targets))
        ]
        for load in pair:
            load.start()
        every.append(pair)
    return every


def table_kernel(
    z, state_hbm, slope_hbm, sites_ref, low_ref, high_ref, col_ref, row_ref,
    mid_scr, rows_scr, site_scr, state_ref, slope_ref, sem,
):
    loads = fetches(z, (state_hbm, slope_hbm), (state_ref, slope_ref), sem)
    part = lax.axis_index("sys")
    span = z.slots * z.modes
    lane = iota((1, z.levels), 1)
    for k in range(z.modes):
        site_scr[k : k + 1, :] = jnp.where(lane == sites_ref[k], 1.0, 0.0)
    at_site = site_scr[: z.modes, :].astype(BF16)
    rows_scr[...] = jnp.zeros_like(rows_scr)
    for g in range(z.slots):
        for load in loads[g]:
            load.wait()
        mid = state_ref[g] + (0.5 * step_size) * slope_ref[g]
        mid_scr[g] = mid
        for third, values in enumerate(thirds(mid)):
            at = third * span + g * z.modes
            col_ref[at : at + z.modes, :] = dot_nt(at_site, values).astype(BF16)
        for c in range(2):
            start = c * z.rows
            low_ref[g, c] = mid_scr[g, start : start + z.band, :]
            high_ref[g, c] = mid_scr[g, start + z.rows - z.band : start + z.rows, :]
            for k in range(z.block_modes):
                local = sites_ref[part * z.block_modes + k] - part * z.rows
                at = g * z.block_modes + k
                rows_scr[at : at + 1, c * z.levels : (c + 1) * z.levels] = mid_scr[
                    g, pl.ds(start + local, 1), :
                ]
    for third, values in enumerate(thirds(rows_scr[...])):
        row_ref[third * z.row_pad : (third + 1) * z.row_pad, :] = values


def answer_kernel(z, ask_ref, col_ref, row_ref, out_ref):
    part = lax.axis_index("sys")
    span = z.slots * z.modes
    low = part * z.block_modes
    asked = ask_ref[...]
    columns = []
    row_at = [jnp.full((z.tiers, 1), -1, jnp.int32) for _ in range(z.row_cap)]
    used = jnp.zeros((z.tiers, 1), jnp.int32)
    for p in range(z.cap):
        target = asked[:, 2 * p : 2 * p + 1]
        mode = asked[:, 2 * p + 1 : 2 * p + 2]
        columns.append(as_bf16(target * z.modes + mode == iota((z.tiers, span), 1)))
        inside = jnp.logical_and(mode >= low, mode < low + z.block_modes)
        where_row = target * z.block_modes + (mode - low)
        for j in range(z.row_cap):
            take = jnp.logical_and(inside, used == j)
            row_at[j] = jnp.where(take, where_row, row_at[j])
        used = used + jnp.where(inside, 1, 0)
    chosen = jnp.concatenate(columns, axis=0)
    found = dot_nn(chosen, col_ref[:span, :])
    for third in (1, 2):
        found = found + dot_nn(chosen, col_ref[third * span : (third + 1) * span, :])
    for p in range(z.cap):
        out_ref[pl.ds(p, z.tiers, stride=z.message), :] = found[p * z.tiers : (p + 1) * z.tiers, :]
    lanes = iota((z.tiers, z.row_pad), 1)
    chosen = jnp.concatenate([as_bf16(at == lanes) for at in row_at], axis=0)
    found = dot_nn(chosen, row_ref[: z.row_pad, :])
    for third in (1, 2):
        found = found + dot_nn(chosen, row_ref[third * z.row_pad : (third + 1) * z.row_pad, :])
    for j in range(z.row_cap):
        for t in range(z.lane_tiles):
            at = z.cap + j * z.lane_tiles + t
            out_ref[pl.ds(at, z.tiers, stride=z.message), :] = found[
                j * z.tiers : (j + 1) * z.tiers, t * LANES : (t + 1) * LANES
            ]


def choose_kernel(
    z, links_ref, counts_ref, coef_ref, rate_ref, col_ref, row_ref, col_coef_ref, row_coef_ref, damp_ref
):
    part = lax.axis_index("sys")
    low = part * z.block_modes
    earlier = earlier_table(z.per_slot)
    ones = jnp.ones((z.per_slot, z.per_slot), BF16)
    seen = jnp.zeros((z.tiers, z.per_slot), F32)
    seen_rows = jnp.zeros((z.tiers, z.per_slot), F32)
    counts = as_column(counts_ref[...], z.tiers)
    rate = as_column(rate_ref[...], z.modes)
    coefs = [as_column(coef_ref[c : c + 1, :], z.modes) for c in range(2)]
    total = z.slots * z.modes
    for g in range(z.slots):
        hit, holder, target = holders_of(z, links_ref, g)
        mode = links_ref[1, g : g + 1, :]
        kind = links_ref[2, g : g + 1, :]
        level = links_ref[3, g : g + 1, :]
        rank = rank_of(hit, seen, earlier)
        seen = seen + dot_nn(as_bf16(hit), ones)
        inside = jnp.logical_and(mode >= low, mode < low + z.block_modes)
        hit_rows = jnp.logical_and(hit, inside)
        row_rank = rank_of(hit_rows, seen_rows, earlier)
        seen_rows = seen_rows + dot_nn(as_bf16(hit_rows), ones)
        live = target < jnp.sum(jnp.where(hit, counts, 0), axis=0, keepdims=True)
        scale = jnp.where(kind == 1, level, 1)
        here = as_bf16(iota((z.cap * z.tiers, z.per_slot), 0) == rank * z.tiers + holder)
        here_row = as_bf16(
            iota((z.row_cap * z.tiers, z.per_slot), 0) == row_rank * z.tiers + holder
        )
        modes = iota((z.modes, z.per_slot), 0)
        group = iota((z.group, z.per_slot), 0)
        for way in range(2):
            wanted = jnp.logical_and(kind == way, live)
            chosen = jnp.where(jnp.logical_and(modes == mode, wanted), scale, 0)
            at = way * total + g * z.modes
            col_ref[at : at + z.modes, :] = dot_nt(
                chosen.astype(F32).astype(BF16), here
            ).astype(BF16)
            own = jnp.logical_and(group + low == mode, jnp.logical_and(inside, wanted))
            at = (way * z.slots + g) * z.group
            row_ref[at : at + z.group, :] = dot_nt(
                jnp.where(own, scale, 0).astype(F32).astype(BF16), here_row
            )
        falling = jnp.where(jnp.logical_and(modes == mode, kind == 1), level, 0).astype(F32)
        amount = jnp.sum(falling, axis=1, keepdims=True) * rate
        damp_ref[g] = jnp.broadcast_to(jnp.sum(amount, axis=0, keepdims=True), (8, LANES))
    for c in range(2):
        col_coef_ref[c] = jnp.broadcast_to(coefs[c], (z.modes, LANES))
        mine = jnp.where(
            iota((z.group, z.modes), 0) + low == iota((z.group, z.modes), 1),
            coef_ref[c : c + 1, :],
            0.0,
        )
        mine = jnp.where(iota((z.group, z.modes), 0) < z.block_modes, mine, 0.0)
        row_coef_ref[c] = jnp.broadcast_to(
            jnp.sum(mine, axis=1, keepdims=True), (z.group, LANES)
        )


def band_kernel(
    z, state_hbm, slope_hbm, bands_ref, damp_ref, out_ref, base_hbm, down_ref, wide, spread, across_ref,
    state_ref, slope_ref, base_ref, sem, base_sem,
):
    part = lax.axis_index("sys")
    loads = fetches(z, (state_hbm, slope_hbm), (state_ref, slope_ref), sem)
    taps = 2 * z.band + 1
    across_ref[...] = jnp.zeros_like(across_ref)
    lane = iota((1, z.levels), 1)
    for t in range(taps):
        offset = t - z.band
        row = bands_ref[abs(offset) : abs(offset) + 1, :]
        if offset < 0:
            row = jnp.where(lane >= -offset, pltpu.roll(row, -offset, 1), 0.0)
        elif offset > 0:
            row = jnp.where(lane < z.levels - offset, row, 0.0)
        across_ref[t : t + 1, :] = row
    own = as_bf16(
        iota((z.rows, z.levels), 0) + part * z.rows == iota((z.rows, z.levels), 1)
    )
    down = jnp.zeros((z.rows, across_ref.shape[0]), F32)
    for values in thirds(across_ref[...]):
        down = down + dot_nt(own, values)
    down_ref[...] = down
    for t in range(taps):
        spread[t] = jnp.broadcast_to(down[:, t : t + 1], (z.rows, LANES))
    tiles = z.levels // LANES
    wide[0 : z.band, :] = jnp.zeros((z.band, z.levels), F32)
    wide[z.band + z.rows :, :] = jnp.zeros((z.band, z.levels), F32)
    for g in range(z.slots):
        for load in loads[g]:
            load.wait()
        damp = damp_ref[g, 0:1, 0:1]
        fields = []
        for c in range(2):
            rows = slice(c * z.rows, (c + 1) * z.rows)
            base_ref[g, rows, :] = state_ref[g, rows, :] + (step_size / 6.0) * slope_ref[g, rows, :]
            fields.append(state_ref[g, rows, :] + (0.5 * step_size) * slope_ref[g, rows, :])
        pltpu.make_async_copy(base_ref.at[g], base_hbm.at[g], base_sem.at[g]).start()
        for c in range(2):
            field = fields[c]
            wide[z.band : z.band + z.rows, :] = field
            summed = across_ref[z.band : z.band + 1, :] * field
            for t in range(taps):
                if t != z.band:
                    moved = pltpu.roll(field, (z.band - t) % z.levels, 1)
                    summed = summed + across_ref[t : t + 1, :] * moved
            sides = []
            for q in range(tiles):
                lanes = slice(q * LANES, (q + 1) * LANES)
                total = spread[0] * wide[0 : z.rows, lanes]
                for t in range(1, taps):
                    total = total + spread[t] * wide[t : t + z.rows, lanes]
                sides.append(total)
            commuted = jnp.concatenate(sides, axis=1) - summed
            other = 1 - c
            sign = 1.0 if c == 1 else -1.0
            out_ref[g, other * z.rows : (other + 1) * z.rows, :] = (
                sign * commuted - damp * fields[other]
            )
    for g in range(z.slots):
        pltpu.make_async_copy(base_ref.at[g], base_hbm.at[g], base_sem.at[g]).wait()


def edge_kernel(z, low_ref, high_ref, down_ref, out_ref, wide):
    band = z.band
    nothing = jnp.zeros((band, z.levels), F32)
    down = down_ref[...]
    last = z.rows - band
    for g in range(z.slots):
        for c in range(2):
            sign = 1.0 if c == 1 else -1.0
            wide[0:band, :] = low_ref[g, c]
            wide[band : 2 * band, :] = nothing
            wide[2 * band : 3 * band, :] = high_ref[g, c]
            top = nothing
            bottom = nothing
            for t in range(band):
                top = top + down[0:band, t : t + 1] * wide[t : t + band, :]
                bottom = (
                    bottom
                    + down[last:, band + 1 + t : band + 2 + t]
                    * wide[band + 1 + t : 2 * band + 1 + t, :]
                )
            out_ref[g, 1 - c, 0] = sign * top
            out_ref[g, 1 - c, 1] = sign * bottom


def apply_kernel(
    z, got_ref, col_ref, row_ref, col_coef_ref, row_coef_ref, deriv_hbm, edge_ref, base_hbm,
    counts_ref, sites_ref, next_ref, sum_ref, site_scr, rows_scr, next_scr, sum_scr, deriv_ref,
    base_ref, sem, load_sem,
):
    loads = fetches(z, (deriv_hbm, base_hbm), (deriv_ref, base_ref), load_sem)
    part = lax.axis_index("sys")
    tier = lax.axis_index("tier")
    lane = iota((1, z.levels), 1)
    for k in range(z.modes):
        site_scr[k : k + 1, :] = jnp.where(lane == sites_ref[k], 1.0, 0.0)
    at_site = site_scr[: z.modes, :].astype(BF16)
    total = z.slots * z.modes
    pieces = jnp.concatenate(
        [
            jnp.concatenate(
                [
                    got_ref[pl.ds(z.cap + j * z.lane_tiles + t, z.tiers, stride=z.message), :]
                    for t in range(z.lane_tiles)
                ],
                axis=1,
            )
            for j in range(z.row_cap)
        ],
        axis=0,
    )
    found = picked(row_ref[...].astype(BF16), pieces)
    half = z.slots * z.group
    up, down = found[:half], found[half:]
    real = jnp.concatenate([row_coef_ref[0, :, 0:1]] * z.slots, axis=0)
    imag = jnp.concatenate([row_coef_ref[1, :, 0:1]] * z.slots, axis=0)
    turned = up + real * down
    straight = imag * down
    rows_scr[0] = straight[:, : z.levels] + turned[:, z.levels :]
    rows_scr[1] = straight[:, z.levels :] - turned[:, : z.levels]
    pieces = thirds(
        jnp.concatenate(
            [got_ref[pl.ds(p, z.tiers, stride=z.message), :] for p in range(z.cap)], axis=0
        )
    )
    sign = jnp.where(iota((1, 2 * z.rows), 1) < z.rows, -1.0, 1.0)
    for g in range(z.slots):
        up = jnp.zeros((z.modes, 2 * z.rows), F32)
        down = up
        for values in pieces:
            up = up + dot_nn(col_ref[g * z.modes : (g + 1) * z.modes, :], values)
            down = down + dot_nn(
                col_ref[total + g * z.modes : total + (g + 1) * z.modes, :], values
            )
        cols = col_coef_ref[1] * down + sign * pltpu.roll(up + col_coef_ref[0] * down, z.rows, 1)
        added = jnp.zeros((2 * z.rows, z.levels), F32)
        for values in thirds(cols):
            added = added + dot_tn(values, at_site)
        for load in loads[g]:
            load.wait()
        next_scr[g] = deriv_ref[g] + added
        for c in range(2):
            for side in range(2):
                start = c * z.rows + side * (z.rows - z.band)
                at = slice(start, start + z.band)
                next_scr[g, at, :] = next_scr[g, at, :] + edge_ref[g, c, side]
        for k in range(z.block_modes):
            local = sites_ref[part * z.block_modes + k] - part * z.rows
            for c in range(2):
                at = pl.ds(c * z.rows + local, 1)
                row = g * z.group + k
                next_scr[g, at, :] = next_scr[g, at, :] + rows_scr[c, row : row + 1, :]
        live = jnp.where(g < counts_ref[tier], 1.0, 0.0)
        slope_next = next_scr[g] * live
        next_scr[g] = slope_next
        sum_scr[g] = (base_ref[g] + (step_size / 3.0) * slope_next) * live
        pltpu.make_async_copy(next_scr.at[g], next_ref.at[g], sem.at[0, g]).start()
        pltpu.make_async_copy(sum_scr.at[g], sum_ref.at[g], sem.at[1, g]).start()
    for g in range(z.slots):
        pltpu.make_async_copy(next_scr.at[g], next_ref.at[g], sem.at[0, g]).wait()
        pltpu.make_async_copy(sum_scr.at[g], sum_ref.at[g], sem.at[1, g]).wait()


def call(kernel, z, name, args, in_specs, outs, scratch=(), out_specs=None, micros=1, aliases=()):
    return pl.pallas_call(
        functools.partial(kernel, z),
        out_shape=outs,
        in_specs=in_specs,
        out_specs=[VMEM] * len(outs) if out_specs is None else out_specs,
        scratch_shapes=list(scratch),
        name=name,
        input_output_aliases=dict(aliases),
        compiler_params=pltpu.CompilerParams(vmem_limit_bytes=int(vmem_limits.get(name, 16) * mib)),
        cost_estimate=pl.CostEstimate(
            flops=int(micros * 1e6), bytes_accessed=int(micros * 1e5), transcendentals=0
        ),
    )(*args)


def neighbours(low_edge, high_edge):
    count = lax.axis_size("sys")
    forward = [(i, i + 1) for i in range(count - 1)]
    backward = [(target, source) for source, target in forward]
    return lax.ppermute(high_edge, "sys", forward), lax.ppermute(low_edge, "sys", backward)


def shards(state, slope, counts, links, mode_site, mode_coef, mode_rate, h_bands):
    z = Sizes(state, links, h_bands, lax.axis_size("tier"), lax.axis_size("sys"))
    shape = jax.ShapeDtypeStruct
    flat = (z.slots, 2 * z.rows, z.levels)
    state_flat = state.reshape(flat)
    slope_flat = slope.reshape(flat)
    (ask,) = call(
        ask_kernel, z, "ask", (links,), [VMEM], [shape((z.tiers, z.ask), jnp.int32)]
    )
    asked = lax.all_to_all(
        ask.reshape(z.tiers, 1, z.ask), "tier", split_axis=0, concat_axis=0, tiled=True
    ).reshape(z.tiers, z.ask)
    edge = (z.slots, 2, z.band, z.levels)
    low_edge, high_edge, col_table, row_table = call(
        table_kernel,
        z,
        "tables",
        (state_flat, slope_flat, mode_site),
        [HBM, HBM, SMEM],
        [
            shape(edge, F32),
            shape(edge, F32),
            shape((3 * z.slots * z.modes, 2 * z.rows), BF16),
            shape((3 * z.row_pad, 2 * z.levels), BF16),
        ],
        [
            pltpu.VMEM(flat, F32),
            pltpu.VMEM((z.row_pad, 2 * z.levels), F32),
            pltpu.VMEM((round_up(z.modes, 16), z.levels), F32),
            pltpu.VMEM(flat, F32),
            pltpu.VMEM(flat, F32),
            pltpu.SemaphoreType.DMA((2, z.slots)),
        ],
        micros=3,
    )
    (answer,) = call(
        answer_kernel,
        z,
        "answer",
        (asked, col_table, row_table),
        [VMEM] * 3,
        [shape((z.tiers * z.message, LANES), F32)],
    )
    got = lax.all_to_all(
        answer.reshape(z.tiers, 1, z.message * LANES),
        "tier",
        split_axis=0,
        concat_axis=0,
        tiled=True,
    ).reshape(z.tiers * z.message, LANES)
    low_edge, high_edge, answer_kept = lax.optimization_barrier((low_edge, high_edge, answer))
    above, below = neighbours(low_edge, high_edge)
    col_choice, row_choice, col_coef, row_coef, damp = call(
        choose_kernel,
        z,
        "choose",
        (links, counts[None], mode_coef, mode_rate[None]),
        [VMEM] * 4,
        [
            shape((2 * z.slots * z.modes, z.cap * z.tiers), BF16),
            shape((2 * z.slots * z.group, z.row_cap * z.tiers), F32),
            shape((2, z.modes, LANES), F32),
            shape((2, z.group, LANES), F32),
            shape((z.slots, 8, LANES), F32),
        ],
        micros=2,
    )
    taps = round_up(2 * z.band + 1, 16)
    deriv, base, down = call(
        band_kernel,
        z,
        "band",
        (state_flat, slope_flat, h_bands, damp),
        [HBM, HBM, VMEM, VMEM],
        [shape(flat, F32), shape(flat, F32), shape((z.rows, taps), F32)],
        [
            pltpu.VMEM((z.rows + 2 * z.band, z.levels), F32),
            pltpu.VMEM((2 * z.band + 1, z.rows, LANES), F32),
            pltpu.VMEM((taps, z.levels), F32),
            pltpu.VMEM(flat, F32),
            pltpu.VMEM(flat, F32),
            pltpu.VMEM(flat, F32),
            pltpu.SemaphoreType.DMA((2, z.slots)),
            pltpu.SemaphoreType.DMA((z.slots,)),
        ],
        out_specs=[VMEM, HBM, VMEM],
        micros=5,
    )
    (edges,) = call(
        edge_kernel,
        z,
        "edges",
        (above, below, down),
        [VMEM] * 3,
        [shape((z.slots, 2, 2, z.band, z.levels), F32)],
        [pltpu.VMEM((3 * z.band, z.levels), F32)],
    )
    slope_next, partial_sum = call(
        apply_kernel,
        z,
        "apply",
        (got, col_choice, row_choice, col_coef, row_coef, deriv, edges, base, counts, mode_site),
        [VMEM] * 5 + [HBM, VMEM, HBM] + [SMEM] * 2,
        [shape(flat, F32), shape(flat, F32)],
        [
            pltpu.VMEM((round_up(z.modes, 8), z.levels), F32),
            pltpu.VMEM((2, z.slots * z.group, z.levels), F32),
            pltpu.VMEM(flat, F32),
            pltpu.VMEM(flat, F32),
            pltpu.VMEM(flat, F32),
            pltpu.VMEM(flat, F32),
            pltpu.SemaphoreType.DMA((2, z.slots)),
            pltpu.SemaphoreType.DMA((2, z.slots)),
        ],
        out_specs=[HBM, HBM],
        aliases=((5, 0), (7, 1)),
        micros=4,
    )
    return slope_next.reshape(state.shape), partial_sum.reshape(state.shape)


def solution(mesh):
    in_specs = (
        P("tier", None, "sys", None),
        P("tier", None, "sys", None),
        P(),
        P(None, "tier", None),
        P(),
        P(),
        P(),
        P(),
    )
    out_specs = (P("tier", None, "sys", None), P("tier", None, "sys", None))
    return jax.shard_map(shards, mesh=mesh, in_specs=in_specs, out_specs=out_specs, check_vma=False)
```

```python
import functools

import jax
import jax.numpy as jnp
from jax import lax
from jax.experimental import pallas as pl
from jax.experimental.pallas import tpu as pltpu
from jax.sharding import PartitionSpec as P

step_size = 0.05
LANES = 128
mib = 1024 * 1024
vmem_limits = {"tables": 16, "band": 16, "apply": 16}
BF16 = jnp.bfloat16
F32 = jnp.float32
VMEM = pl.BlockSpec(memory_space=pltpu.VMEM)
SMEM = pl.BlockSpec(memory_space=pltpu.SMEM)
HBM = pl.BlockSpec(memory_space=pltpu.HBM)


def iota(shape, dim):
    return lax.broadcasted_iota(jnp.int32, shape, dim)


def round_up(value, multiple):
    return -(-value // multiple) * multiple


def dot_nn(a, b):
    return lax.dot_general(a, b, (((1,), (0,)), ((), ())), preferred_element_type=F32)


def dot_nt(a, b):
    return lax.dot_general(a, b, (((1,), (1,)), ((), ())), preferred_element_type=F32)


def dot_tn(a, b):
    return lax.dot_general(a, b, (((0,), (0,)), ((), ())), preferred_element_type=F32)


def thirds(x):
    first = x.astype(BF16)
    rest = x - first.astype(F32)
    second = rest.astype(BF16)
    third = (rest - second.astype(F32)).astype(BF16)
    return first, second, third


def halves(x):
    first = x.astype(BF16)
    return first, (x - first.astype(F32)).astype(BF16)


def picked(chooser, values):
    first, second = halves(values)
    return dot_nn(chooser, first) + dot_nn(chooser, second)


def as_bf16(mask):
    return jnp.where(mask, 1.0, 0.0).astype(BF16)


def as_column(row, size):
    diagonal = iota((size, size), 0) == iota((size, size), 1)
    return jnp.sum(jnp.where(diagonal, row, jnp.zeros((), row.dtype)), axis=1, keepdims=True)


class Sizes:
    def __init__(self, state, links, h_bands, tiers, parts):
        self.slots = state.shape[0]
        self.rows = state.shape[2]
        self.levels = state.shape[3]
        self.band = h_bands.shape[0] - 1
        self.per_slot = links.shape[2]
        self.tiers = tiers
        self.parts = parts
        self.modes = self.per_slot // 2
        self.block_modes = self.modes // parts
        total = self.slots * self.per_slot
        self.cap = total // tiers
        self.row_cap = 2 * ((self.slots * self.block_modes + tiers - 1) // tiers)
        self.lane_tiles = 2 * self.levels // LANES
        self.message = self.cap + self.row_cap * self.lane_tiles
        self.ask = round_up(2 * self.cap, 16)
        self.shift = self.slots.bit_length() - 1
        self.row_pad = round_up(self.slots * self.block_modes, 16)
        self.group = round_up(self.block_modes, 8)


def holders_of(z, links_ref, g):
    neighbour = links_ref[0, g : g + 1, :]
    holder = lax.shift_right_logical(neighbour, z.shift)
    target = lax.bitwise_and(neighbour, z.slots - 1)
    hit = holder == iota((z.tiers, z.per_slot), 0)
    return hit, holder, target


def earlier_table(size):
    return as_bf16(iota((size, size), 0) < iota((size, size), 1))


def rank_of(hit, seen, earlier):
    before = dot_nn(as_bf16(hit), earlier) + seen
    return jnp.sum(jnp.where(hit, before, 0.0), axis=0, keepdims=True).astype(jnp.int32)


def ask_kernel(z, links_ref, out_ref):
    earlier = earlier_table(z.per_slot)
    ones = jnp.ones((z.per_slot, z.per_slot), BF16)
    seen = jnp.zeros((z.tiers, z.per_slot), F32)
    table = jnp.zeros((z.tiers, z.ask), F32)
    field = iota((z.ask, z.per_slot), 0)
    for g in range(z.slots):
        hit, _, target = holders_of(z, links_ref, g)
        mode = links_ref[1, g : g + 1, :]
        rank = rank_of(hit, seen, earlier)
        value = jnp.where(lax.bitwise_and(field, 1) == 0, target, mode)
        value = jnp.where(lax.shift_right_logical(field, 1) == rank, value, 0)
        chosen = as_bf16(hit)
        table = table + dot_nt(chosen, value.astype(F32).astype(BF16))
        seen = seen + dot_nn(chosen, ones)
    out_ref[...] = table.astype(jnp.int32)


def table_kernel(
    z, state_ref, slope_ref, sites_ref, low_ref, high_ref, col_ref, row_ref,
    mid_scr, rows_scr, site_scr,
):
    part = lax.axis_index("sys")
    span = z.slots * z.modes
    lane = iota((1, z.levels), 1)
    for k in range(z.modes):
        site_scr[k : k + 1, :] = jnp.where(lane == sites_ref[k], 1.0, 0.0)
    at_site = site_scr[: z.modes, :].astype(BF16)
    rows_scr[...] = jnp.zeros_like(rows_scr)
    for g in range(z.slots):
        mid = state_ref[g] + (0.5 * step_size) * slope_ref[g]
        mid_scr[g] = mid
        for third, values in enumerate(thirds(mid)):
            at = third * span + g * z.modes
            col_ref[at : at + z.modes, :] = dot_nt(at_site, values).astype(BF16)
        for c in range(2):
            start = c * z.rows
            low_ref[g, c] = mid_scr[g, start : start + z.band, :]
            high_ref[g, c] = mid_scr[g, start + z.rows - z.band : start + z.rows, :]
            for k in range(z.block_modes):
                local = sites_ref[part * z.block_modes + k] - part * z.rows
                at = g * z.block_modes + k
                rows_scr[at : at + 1, c * z.levels : (c + 1) * z.levels] = mid_scr[
                    g, pl.ds(start + local, 1), :
                ]
    for third, values in enumerate(thirds(rows_scr[...])):
        row_ref[third * z.row_pad : (third + 1) * z.row_pad, :] = values


def answer_kernel(z, ask_ref, col_ref, row_ref, out_hbm, out_scr, sem):
    part = lax.axis_index("sys")
    span = z.slots * z.modes
    low = part * z.block_modes
    asked = ask_ref[...]
    columns = []
    row_at = [jnp.full((z.tiers, 1), -1, jnp.int32) for _ in range(z.row_cap)]
    used = jnp.zeros((z.tiers, 1), jnp.int32)
    for p in range(z.cap):
        target = asked[:, 2 * p : 2 * p + 1]
        mode = asked[:, 2 * p + 1 : 2 * p + 2]
        columns.append(as_bf16(target * z.modes + mode == iota((z.tiers, span), 1)))
        inside = jnp.logical_and(mode >= low, mode < low + z.block_modes)
        where_row = target * z.block_modes + (mode - low)
        for j in range(z.row_cap):
            take = jnp.logical_and(inside, used == j)
            row_at[j] = jnp.where(take, where_row, row_at[j])
        used = used + jnp.where(inside, 1, 0)
    lanes = iota((z.tiers, z.row_pad), 1)
    row_choice = [as_bf16(at == lanes) for at in row_at]
    parts = 2
    size = z.tiers // parts
    copies = []
    for part in range(parts):
        mine = slice(part * size, (part + 1) * size)
        start = part * size * z.message
        chosen = jnp.concatenate([choice[mine] for choice in row_choice], axis=0)
        found = dot_nn(chosen, row_ref[: z.row_pad, :])
        for third in (1, 2):
            found = found + dot_nn(
                chosen, row_ref[third * z.row_pad : (third + 1) * z.row_pad, :]
            )
        for j in range(z.row_cap):
            for t in range(z.lane_tiles):
                at = start + z.cap + j * z.lane_tiles + t
                out_scr[pl.ds(at, size, stride=z.message), :] = found[
                    j * size : (j + 1) * size, t * LANES : (t + 1) * LANES
                ]
        chosen = jnp.concatenate([choice[mine] for choice in columns], axis=0)
        found = dot_nn(chosen, col_ref[:span, :])
        for third in (1, 2):
            found = found + dot_nn(chosen, col_ref[third * span : (third + 1) * span, :])
        for p in range(z.cap):
            out_scr[pl.ds(start + p, size, stride=z.message), :] = found[
                p * size : (p + 1) * size, :
            ]
        block = pl.ds(start, size * z.message)
        copies.append(
            pltpu.make_async_copy(out_scr.at[block], out_hbm.at[block], sem.at[part])
        )
        copies[-1].start()
    for copy in copies:
        copy.wait()


def choose_kernel(
    z, links_ref, counts_ref, coef_ref, rate_ref, own_ref, sites_ref,
    col_ref, row_ref, col_coef_ref, row_coef_ref, damp_ref, at_ref, site_scr,
):
    part = lax.axis_index("sys")
    tier = lax.axis_index("tier")
    lane = iota((1, z.levels), 1)
    for k in range(z.modes):
        site_scr[k : k + 1, :] = jnp.where(lane == sites_ref[k], 1.0, 0.0)
    at_ref[...] = site_scr[: z.modes, :].astype(BF16)
    low = part * z.block_modes
    earlier = earlier_table(z.per_slot)
    ones = jnp.ones((z.per_slot, z.per_slot), BF16)
    seen = jnp.zeros((z.tiers, z.per_slot), F32)
    seen_rows = jnp.zeros((z.tiers, z.per_slot), F32)
    counts = as_column(counts_ref[...], z.tiers)
    rate = as_column(rate_ref[...], z.modes)
    coefs = [as_column(coef_ref[c : c + 1, :], z.modes) for c in range(2)]
    total = z.slots * z.modes
    for g in range(z.slots):
        hit, holder, target = holders_of(z, links_ref, g)
        mode = links_ref[1, g : g + 1, :]
        kind = links_ref[2, g : g + 1, :]
        level = links_ref[3, g : g + 1, :]
        rank = rank_of(hit, seen, earlier)
        seen = seen + dot_nn(as_bf16(hit), ones)
        inside = jnp.logical_and(mode >= low, mode < low + z.block_modes)
        hit_rows = jnp.logical_and(hit, inside)
        row_rank = rank_of(hit_rows, seen_rows, earlier)
        seen_rows = seen_rows + dot_nn(as_bf16(hit_rows), ones)
        live = target < jnp.sum(jnp.where(hit, counts, 0), axis=0, keepdims=True)
        live = jnp.logical_and(live, own_ref[tier] > g)
        scale = jnp.where(kind == 1, level, 1)
        here = as_bf16(iota((z.cap * z.tiers, z.per_slot), 0) == rank * z.tiers + holder)
        here_row = as_bf16(
            iota((z.row_cap * z.tiers, z.per_slot), 0) == row_rank * z.tiers + holder
        )
        modes = iota((z.modes, z.per_slot), 0)
        group = iota((z.group, z.per_slot), 0)
        for way in range(2):
            wanted = jnp.logical_and(kind == way, live)
            chosen = jnp.where(jnp.logical_and(modes == mode, wanted), scale, 0)
            at = way * total + g * z.modes
            col_ref[at : at + z.modes, :] = dot_nt(
                chosen.astype(F32).astype(BF16), here
            ).astype(BF16)
            own = jnp.logical_and(group + low == mode, jnp.logical_and(inside, wanted))
            at = (way * z.slots + g) * z.group
            row_ref[at : at + z.group, :] = dot_nt(
                jnp.where(own, scale, 0).astype(F32).astype(BF16), here_row
            )
        falling = jnp.where(jnp.logical_and(modes == mode, kind == 1), level, 0).astype(F32)
        amount = jnp.sum(falling, axis=1, keepdims=True) * rate
        damp_ref[g] = jnp.broadcast_to(jnp.sum(amount, axis=0, keepdims=True), (8, LANES))
    for c in range(2):
        col_coef_ref[c] = jnp.broadcast_to(coefs[c], (z.modes, LANES))
        mine = jnp.where(
            iota((z.group, z.modes), 0) + low == iota((z.group, z.modes), 1),
            coef_ref[c : c + 1, :],
            0.0,
        )
        mine = jnp.where(iota((z.group, z.modes), 0) < z.block_modes, mine, 0.0)
        row_coef_ref[c] = jnp.broadcast_to(
            jnp.sum(mine, axis=1, keepdims=True), (z.group, LANES)
        )


def band_kernel(
    z, state_ref, slope_ref, low_ref, high_ref, bands_ref, damp_ref, counts_ref,
    out_ref, wide, spread, across_ref,
):
    part = lax.axis_index("sys")
    own = counts_ref[lax.axis_index("tier")]
    taps = 2 * z.band + 1
    across_ref[...] = jnp.zeros_like(across_ref)
    lane = iota((1, z.levels), 1)
    for t in range(taps):
        offset = t - z.band
        row = bands_ref[abs(offset) : abs(offset) + 1, :]
        if offset < 0:
            row = jnp.where(lane >= -offset, pltpu.roll(row, -offset, 1), 0.0)
        elif offset > 0:
            row = jnp.where(lane < z.levels - offset, row, 0.0)
        across_ref[t : t + 1, :] = row
    here = as_bf16(
        iota((z.rows, z.levels), 0) + part * z.rows == iota((z.rows, z.levels), 1)
    )
    down = jnp.zeros((z.rows, across_ref.shape[0]), F32)
    for values in thirds(across_ref[...]):
        down = down + dot_nt(here, values)
    for t in range(taps):
        spread[t] = jnp.broadcast_to(down[:, t : t + 1], (z.rows, LANES))
    tiles = z.levels // LANES
    for g in range(z.slots):
        live = jnp.where(g < own, 1.0, 0.0)
        damp = damp_ref[g, 0:1, 0:1]
        fields = []
        for c in range(2):
            rows = slice(c * z.rows, (c + 1) * z.rows)
            fields.append(state_ref[g, rows, :] + (0.5 * step_size) * slope_ref[g, rows, :])
        for c in range(2):
            field = fields[c]
            wide[0 : z.band, :] = low_ref[g, c]
            wide[z.band : z.band + z.rows, :] = field
            wide[z.band + z.rows :, :] = high_ref[g, c]
            summed = across_ref[z.band : z.band + 1, :] * field
            for t in range(taps):
                if t != z.band:
                    moved = pltpu.roll(field, (z.band - t) % z.levels, 1)
                    summed = summed + across_ref[t : t + 1, :] * moved
            sides = []
            for q in range(tiles):
                lanes = slice(q * LANES, (q + 1) * LANES)
                total = spread[0] * wide[0 : z.rows, lanes]
                for t in range(1, taps):
                    total = total + spread[t] * wide[t : t + z.rows, lanes]
                sides.append(total)
            commuted = jnp.concatenate(sides, axis=1) - summed
            other = 1 - c
            sign = 1.0 if c == 1 else -1.0
            out_ref[g, other * z.rows : (other + 1) * z.rows, :] = (
                live * (sign * commuted - damp * fields[other])
            )


def apply_kernel(
    z, got_ref, col_ref, row_ref, col_coef_ref, row_coef_ref, deriv_hbm, state_ref, slope_ref,
    at_ref, counts_ref, sites_ref, next_ref, sum_ref, rows_scr, next_scr, sum_scr, deriv_ref,
    sem, load_sem,
):
    loads = [
        pltpu.make_async_copy(deriv_hbm.at[g], deriv_ref.at[g], load_sem.at[g])
        for g in range(z.slots)
    ]
    for load in loads:
        load.start()
    part = lax.axis_index("sys")
    tier = lax.axis_index("tier")
    at_site = at_ref[...]
    total = z.slots * z.modes
    pieces = jnp.concatenate(
        [
            jnp.concatenate(
                [
                    got_ref[pl.ds(z.cap + j * z.lane_tiles + t, z.tiers, stride=z.message), :]
                    for t in range(z.lane_tiles)
                ],
                axis=1,
            )
            for j in range(z.row_cap)
        ],
        axis=0,
    )
    found = picked(row_ref[...].astype(BF16), pieces)
    half = z.slots * z.group
    up, down = found[:half], found[half:]
    real = jnp.concatenate([row_coef_ref[0, :, 0:1]] * z.slots, axis=0)
    imag = jnp.concatenate([row_coef_ref[1, :, 0:1]] * z.slots, axis=0)
    turned = up + real * down
    straight = imag * down
    rows_scr[0] = straight[:, : z.levels] + turned[:, z.levels :]
    rows_scr[1] = straight[:, z.levels :] - turned[:, : z.levels]
    pieces = jnp.concatenate(
        [got_ref[pl.ds(p, z.tiers, stride=z.message), :] for p in range(z.cap)], axis=0
    )
    found = picked(col_ref[...], pieces)
    sign = jnp.where(iota((1, 2 * z.rows), 1) < z.rows, -1.0, 1.0)
    for g in range(z.slots):
        up = found[g * z.modes : (g + 1) * z.modes]
        down = found[total + g * z.modes : total + (g + 1) * z.modes]
        cols = col_coef_ref[1] * down + sign * pltpu.roll(up + col_coef_ref[0] * down, z.rows, 1)
        first, second = halves(cols)
        added = dot_tn(first, at_site) + dot_tn(second, at_site)
        loads[g].wait()
        next_scr[g] = deriv_ref[g] + added
        for k in range(z.block_modes):
            local = sites_ref[part * z.block_modes + k] - part * z.rows
            for c in range(2):
                at = pl.ds(c * z.rows + local, 1)
                row = g * z.group + k
                next_scr[g, at, :] = next_scr[g, at, :] + rows_scr[c, row : row + 1, :]
        pltpu.make_async_copy(next_scr.at[g], next_ref.at[g], sem.at[0, g]).start()
        live = jnp.where(g < counts_ref[tier], 1.0, 0.0)
        sum_scr[g] = (state_ref[g] + (step_size / 6.0) * slope_ref[g]) * live + (
            step_size / 3.0
        ) * next_scr[g]
        pltpu.make_async_copy(sum_scr.at[g], sum_ref.at[g], sem.at[1, g]).start()
    for g in range(z.slots):
        pltpu.make_async_copy(next_scr.at[g], next_ref.at[g], sem.at[0, g]).wait()
        pltpu.make_async_copy(sum_scr.at[g], sum_ref.at[g], sem.at[1, g]).wait()


def call(kernel, z, name, args, in_specs, outs, scratch=(), out_specs=None, micros=1, aliases=()):
    return pl.pallas_call(
        functools.partial(kernel, z),
        out_shape=outs,
        in_specs=in_specs,
        out_specs=[VMEM] * len(outs) if out_specs is None else out_specs,
        scratch_shapes=list(scratch),
        name=name,
        input_output_aliases=dict(aliases),
        compiler_params=pltpu.CompilerParams(vmem_limit_bytes=int(vmem_limits.get(name, 16) * mib)),
        cost_estimate=pl.CostEstimate(
            flops=int(micros * 1e6), bytes_accessed=int(micros * 1e5), transcendentals=0
        ),
    )(*args)


def neighbours(low_edge, high_edge):
    count = lax.axis_size("sys")
    forward = [(i, i + 1) for i in range(count - 1)]
    backward = [(target, source) for source, target in forward]
    return lax.ppermute(high_edge, "sys", forward), lax.ppermute(low_edge, "sys", backward)


def shards(state, slope, counts, links, mode_site, mode_coef, mode_rate, h_bands):
    z = Sizes(state, links, h_bands, lax.axis_size("tier"), lax.axis_size("sys"))
    shape = jax.ShapeDtypeStruct
    flat = (z.slots, 2 * z.rows, z.levels)
    state_flat = state.reshape(flat)
    slope_flat = slope.reshape(flat)
    (ask,) = call(
        ask_kernel, z, "ask", (links,), [VMEM], [shape((z.tiers, z.ask), jnp.int32)]
    )
    asked = lax.all_to_all(
        ask.reshape(z.tiers, 1, z.ask), "tier", split_axis=0, concat_axis=0, tiled=True
    ).reshape(z.tiers, z.ask)
    edge = (z.slots, 2, z.band, z.levels)
    low_edge, high_edge, col_table, row_table = call(
        table_kernel,
        z,
        "tables",
        (state_flat, slope_flat, mode_site),
        [VMEM, VMEM, SMEM],
        [
            shape(edge, F32),
            shape(edge, F32),
            shape((3 * z.slots * z.modes, 2 * z.rows), BF16),
            shape((3 * z.row_pad, 2 * z.levels), BF16),
        ],
        [
            pltpu.VMEM(flat, F32),
            pltpu.VMEM((z.row_pad, 2 * z.levels), F32),
            pltpu.VMEM((round_up(z.modes, 16), z.levels), F32),
        ],
        micros=3,
    )
    (answer,) = call(
        answer_kernel,
        z,
        "answer",
        (asked, col_table, row_table),
        [VMEM] * 3,
        [shape((z.tiers * z.message, LANES), F32)],
        [pltpu.VMEM((z.tiers * z.message, LANES), F32), pltpu.SemaphoreType.DMA((2,))],
        out_specs=[HBM],
    )
    got = lax.all_to_all(
        answer.reshape(z.tiers, 1, z.message * LANES),
        "tier",
        split_axis=0,
        concat_axis=0,
        tiled=True,
    ).reshape(z.tiers * z.message, LANES)
    low_edge, high_edge, answer_kept = lax.optimization_barrier((low_edge, high_edge, answer))
    above, below = neighbours(low_edge, high_edge)
    col_choice, row_choice, col_coef, row_coef, damp, at_site = call(
        choose_kernel,
        z,
        "choose",
        (links, counts[None], mode_coef, mode_rate[None], counts, mode_site),
        [VMEM] * 4 + [SMEM] * 2,
        [
            shape((2 * z.slots * z.modes, z.cap * z.tiers), BF16),
            shape((2 * z.slots * z.group, z.row_cap * z.tiers), F32),
            shape((2, z.modes, LANES), F32),
            shape((2, z.group, LANES), F32),
            shape((z.slots, 8, LANES), F32),
            shape((z.modes, z.levels), BF16),
        ],
        [pltpu.VMEM((round_up(z.modes, 16), z.levels), F32)],
        micros=2,
    )
    taps = round_up(2 * z.band + 1, 16)
    (deriv,) = call(
        band_kernel,
        z,
        "band",
        (state_flat, slope_flat, above, below, h_bands, damp, counts),
        [VMEM] * 6 + [SMEM],
        [shape(flat, F32)],
        [
            pltpu.VMEM((z.rows + 2 * z.band, z.levels), F32),
            pltpu.VMEM((2 * z.band + 1, z.rows, LANES), F32),
            pltpu.VMEM((taps, z.levels), F32),
        ],
        micros=5,
    )
    slope_next, partial_sum = call(
        apply_kernel,
        z,
        "apply",
        (
            got, col_choice, row_choice, col_coef, row_coef, deriv, state_flat, slope_flat,
            at_site, counts, mode_site,
        ),
        [VMEM] * 5 + [HBM] + [VMEM] * 3 + [SMEM] * 2,
        [shape(flat, F32), shape(flat, F32)],
        [
            pltpu.VMEM((2, z.slots * z.group, z.levels), F32),
            pltpu.VMEM(flat, F32),
            pltpu.VMEM(flat, F32),
            pltpu.VMEM(flat, F32),
            pltpu.SemaphoreType.DMA((2, z.slots)),
            pltpu.SemaphoreType.DMA((z.slots,)),
        ],
        out_specs=[HBM, HBM],
        aliases=((5, 0),),
        micros=4,
    )
    return slope_next.reshape(state.shape), partial_sum.reshape(state.shape)


def solution(mesh):
    in_specs = (
        P("tier", None, "sys", None),
        P("tier", None, "sys", None),
        P(),
        P(None, "tier", None),
        P(),
        P(),
        P(),
        P(),
    )
    out_specs = (P("tier", None, "sys", None), P("tier", None, "sys", None))
    return jax.shard_map(shards, mesh=mesh, in_specs=in_specs, out_specs=out_specs, check_vma=False)
```

```python
import functools

import jax
import jax.numpy as jnp
from jax import lax
from jax.experimental import pallas as pl
from jax.experimental.pallas import tpu as pltpu
from jax.sharding import PartitionSpec as P

step_size = 0.05
LANES = 128
mib = 1024 * 1024
vmem_limits = {"tables": 16, "band": 16, "apply": 16}
BF16 = jnp.bfloat16
F32 = jnp.float32
VMEM = pl.BlockSpec(memory_space=pltpu.VMEM)
SMEM = pl.BlockSpec(memory_space=pltpu.SMEM)
HBM = pl.BlockSpec(memory_space=pltpu.HBM)


def iota(shape, dim):
    return lax.broadcasted_iota(jnp.int32, shape, dim)


def round_up(value, multiple):
    return -(-value // multiple) * multiple


def dot_nn(a, b):
    return lax.dot_general(a, b, (((1,), (0,)), ((), ())), preferred_element_type=F32)


def dot_nt(a, b):
    return lax.dot_general(a, b, (((1,), (1,)), ((), ())), preferred_element_type=F32)


def dot_tn(a, b):
    return lax.dot_general(a, b, (((0,), (0,)), ((), ())), preferred_element_type=F32)


def thirds(x):
    first = x.astype(BF16)
    rest = x - first.astype(F32)
    second = rest.astype(BF16)
    third = (rest - second.astype(F32)).astype(BF16)
    return first, second, third


def halves(x):
    first = x.astype(BF16)
    return first, (x - first.astype(F32)).astype(BF16)


def picked(chooser, values):
    return dot_nn(
        jnp.concatenate([chooser, chooser], axis=1), jnp.concatenate(halves(values), axis=0)
    )


def as_bf16(mask):
    return jnp.where(mask, 1.0, 0.0).astype(BF16)


def as_column(row, size):
    diagonal = iota((size, size), 0) == iota((size, size), 1)
    return jnp.sum(jnp.where(diagonal, row, jnp.zeros((), row.dtype)), axis=1, keepdims=True)


class Sizes:
    def __init__(self, state, links, h_bands, tiers, parts):
        self.slots = state.shape[0]
        self.rows = state.shape[2]
        self.levels = state.shape[3]
        self.band = h_bands.shape[0] - 1
        self.per_slot = links.shape[2]
        self.tiers = tiers
        self.parts = parts
        self.modes = self.per_slot // 2
        self.block_modes = self.modes // parts
        total = self.slots * self.per_slot
        self.cap = total // tiers
        self.row_cap = 2 * ((self.slots * self.block_modes + tiers - 1) // tiers)
        self.lane_tiles = 2 * self.levels // LANES
        self.message = self.cap + self.row_cap * self.lane_tiles
        self.ask = round_up(2 * self.cap, 16)
        self.shift = self.slots.bit_length() - 1
        self.span = round_up(self.slots * self.modes, LANES)
        self.row_pad = round_up(self.slots * self.block_modes, 16)
        self.group = round_up(self.block_modes, 8)


def holders_of(z, links_ref, g):
    neighbour = links_ref[0, g : g + 1, :]
    holder = lax.shift_right_logical(neighbour, z.shift)
    target = lax.bitwise_and(neighbour, z.slots - 1)
    hit = holder == iota((z.tiers, z.per_slot), 0)
    return hit, holder, target


def earlier_table(size):
    return as_bf16(iota((size, size), 0) < iota((size, size), 1))


def rank_of(hit, seen, earlier):
    before = dot_nn(as_bf16(hit), earlier) + seen
    return jnp.sum(jnp.where(hit, before, 0.0), axis=0, keepdims=True).astype(jnp.int32)


def ask_kernel(z, links_ref, out_ref):
    earlier = earlier_table(z.per_slot)
    ones = jnp.ones((z.per_slot, z.per_slot), BF16)
    seen = jnp.zeros((z.tiers, z.per_slot), F32)
    table = jnp.zeros((z.tiers, z.ask), F32)
    field = iota((z.ask, z.per_slot), 0)
    for g in range(z.slots):
        hit, _, target = holders_of(z, links_ref, g)
        mode = links_ref[1, g : g + 1, :]
        rank = rank_of(hit, seen, earlier)
        value = jnp.where(lax.bitwise_and(field, 1) == 0, target, mode)
        value = jnp.where(lax.shift_right_logical(field, 1) == rank, value, 0)
        chosen = as_bf16(hit)
        table = table + dot_nt(chosen, value.astype(F32).astype(BF16))
        seen = seen + dot_nn(chosen, ones)
    out_ref[...] = table.astype(jnp.int32)


def table_kernel(
    z, state_ref, slope_ref, sites_ref, counts_ref, low_ref, high_ref, col_ref, row_ref, mid_ref,
    base_ref, rows_scr, site_scr,
):
    own = counts_ref[lax.axis_index("tier")]
    part = lax.axis_index("sys")
    lane = iota((1, z.levels), 1)
    used = z.slots * z.modes
    for third in range(3):
        if z.span > used:
            col_ref[third * z.span + used : (third + 1) * z.span, :] = jnp.zeros(
                (z.span - used, 2 * z.rows), BF16
            )
    for k in range(z.modes):
        site_scr[k : k + 1, :] = jnp.where(lane == sites_ref[k], 1.0, 0.0)
    at_site = site_scr[: z.modes, :].astype(BF16)
    rows_scr[...] = jnp.zeros_like(rows_scr)
    for g in range(z.slots):
        live = jnp.where(g < own, 1.0, 0.0)
        base_ref[g] = live * (state_ref[g] + (step_size / 6.0) * slope_ref[g])
        mid = state_ref[g] + (0.5 * step_size) * slope_ref[g]
        mid_ref[g] = mid
        for third, values in enumerate(thirds(mid)):
            at = third * z.span + g * z.modes
            col_ref[at : at + z.modes, :] = dot_nt(at_site, values).astype(BF16)
        for c in range(2):
            start = c * z.rows
            low_ref[g, c] = mid_ref[g, start : start + z.band, :]
            high_ref[g, c] = mid_ref[g, start + z.rows - z.band : start + z.rows, :]
            for k in range(z.block_modes):
                local = sites_ref[part * z.block_modes + k] - part * z.rows
                at = g * z.block_modes + k
                rows_scr[at : at + 1, c * z.levels : (c + 1) * z.levels] = mid_ref[
                    g, pl.ds(start + local, 1), :
                ]
    for third, values in enumerate(thirds(rows_scr[...])):
        row_ref[third * z.row_pad : (third + 1) * z.row_pad, :] = values


def answer_kernel(z, ask_ref, col_ref, row_ref, out_ref):
    part = lax.axis_index("sys")
    low = part * z.block_modes
    asked = ask_ref[...]
    columns = []
    row_at = [jnp.full((z.tiers, 1), -1, jnp.int32) for _ in range(z.row_cap)]
    used = jnp.zeros((z.tiers, 1), jnp.int32)
    lanes = iota((z.tiers, z.span), 1)
    for p in range(z.cap):
        target = asked[:, 2 * p : 2 * p + 1]
        mode = asked[:, 2 * p + 1 : 2 * p + 2]
        columns.append(as_bf16(target * z.modes + mode == lanes))
        inside = jnp.logical_and(mode >= low, mode < low + z.block_modes)
        where_row = target * z.block_modes + (mode - low)
        for j in range(z.row_cap):
            take = jnp.logical_and(inside, used == j)
            row_at[j] = jnp.where(take, where_row, row_at[j])
        used = used + jnp.where(inside, 1, 0)
    lanes = iota((z.tiers, 3 * z.row_pad), 1)
    for third in (2, 1):
        lanes = jnp.where(lanes >= third * z.row_pad, lanes - third * z.row_pad, lanes)
    chosen = jnp.concatenate([as_bf16(at == lanes) for at in row_at], axis=0)
    found = dot_nn(chosen, row_ref[...])
    for j in range(z.row_cap):
        for t in range(z.lane_tiles):
            at = z.cap + j * z.lane_tiles + t
            out_ref[pl.ds(at, z.tiers, stride=z.message), :] = found[
                j * z.tiers : (j + 1) * z.tiers, t * LANES : (t + 1) * LANES
            ]
    chosen = jnp.concatenate(columns, axis=0)
    found = dot_nn(jnp.concatenate([chosen] * 3, axis=1), col_ref[...])
    for p in range(z.cap):
        out_ref[pl.ds(p, z.tiers, stride=z.message), :] = found[p * z.tiers : (p + 1) * z.tiers, :]


def choose_kernel(
    z, links_ref, counts_ref, coef_ref, rate_ref, own_ref, sites_ref,
    col_ref, row_ref, col_coef_ref, row_coef_ref, damp_ref, at_ref, site_scr,
):
    part = lax.axis_index("sys")
    tier = lax.axis_index("tier")
    lane = iota((1, z.levels), 1)
    for k in range(z.modes):
        site_scr[k : k + 1, :] = jnp.where(lane == sites_ref[k], 1.0, 0.0)
    at_ref[...] = site_scr[: z.modes, :].astype(BF16)
    low = part * z.block_modes
    earlier = earlier_table(z.per_slot)
    ones = jnp.ones((z.per_slot, z.per_slot), BF16)
    seen = jnp.zeros((z.tiers, z.per_slot), F32)
    seen_rows = jnp.zeros((z.tiers, z.per_slot), F32)
    counts = as_column(counts_ref[...], z.tiers)
    rate = as_column(rate_ref[...], z.modes)
    coefs = [as_column(coef_ref[c : c + 1, :], z.modes) for c in range(2)]
    total = z.slots * z.modes
    for g in range(z.slots):
        hit, holder, target = holders_of(z, links_ref, g)
        mode = links_ref[1, g : g + 1, :]
        kind = links_ref[2, g : g + 1, :]
        level = links_ref[3, g : g + 1, :]
        rank = rank_of(hit, seen, earlier)
        seen = seen + dot_nn(as_bf16(hit), ones)
        inside = jnp.logical_and(mode >= low, mode < low + z.block_modes)
        hit_rows = jnp.logical_and(hit, inside)
        row_rank = rank_of(hit_rows, seen_rows, earlier)
        seen_rows = seen_rows + dot_nn(as_bf16(hit_rows), ones)
        live = target < jnp.sum(jnp.where(hit, counts, 0), axis=0, keepdims=True)
        live = jnp.logical_and(live, own_ref[tier] > g)
        scale = jnp.where(kind == 1, level, 1)
        here = as_bf16(iota((z.cap * z.tiers, z.per_slot), 0) == rank * z.tiers + holder)
        here_row = as_bf16(
            iota((z.row_cap * z.tiers, z.per_slot), 0) == row_rank * z.tiers + holder
        )
        modes = iota((z.modes, z.per_slot), 0)
        group = iota((z.group, z.per_slot), 0)
        for way in range(2):
            wanted = jnp.logical_and(kind == way, live)
            chosen = jnp.where(jnp.logical_and(modes == mode, wanted), scale, 0)
            at = way * total + g * z.modes
            col_ref[at : at + z.modes, :] = dot_nt(
                chosen.astype(F32).astype(BF16), here
            ).astype(BF16)
            own = jnp.logical_and(group + low == mode, jnp.logical_and(inside, wanted))
            at = (way * z.slots + g) * z.group
            row_ref[at : at + z.group, :] = dot_nt(
                jnp.where(own, scale, 0).astype(F32).astype(BF16), here_row
            )
        falling = jnp.where(jnp.logical_and(modes == mode, kind == 1), level, 0).astype(F32)
        amount = jnp.sum(falling, axis=1, keepdims=True) * rate
        damp_ref[g] = jnp.broadcast_to(jnp.sum(amount, axis=0, keepdims=True), (8, LANES))
    for c in range(2):
        col_coef_ref[c] = jnp.broadcast_to(coefs[c], (z.modes, LANES))
        mine = jnp.where(
            iota((z.group, z.modes), 0) + low == iota((z.group, z.modes), 1),
            coef_ref[c : c + 1, :],
            0.0,
        )
        mine = jnp.where(iota((z.group, z.modes), 0) < z.block_modes, mine, 0.0)
        row_coef_ref[c] = jnp.broadcast_to(
            jnp.sum(mine, axis=1, keepdims=True), (z.group, LANES)
        )


def band_kernel(
    z, mid_ref, low_ref, high_ref, bands_ref, damp_ref, counts_ref, out_ref, wide, spread,
    across_ref, mid_scr,
):
    part = lax.axis_index("sys")
    own = counts_ref[lax.axis_index("tier")]
    taps = 2 * z.band + 1
    across_ref[...] = jnp.zeros_like(across_ref)
    lane = iota((1, z.levels), 1)
    for t in range(taps):
        offset = t - z.band
        row = bands_ref[abs(offset) : abs(offset) + 1, :]
        if offset < 0:
            row = jnp.where(lane >= -offset, pltpu.roll(row, -offset, 1), 0.0)
        elif offset > 0:
            row = jnp.where(lane < z.levels - offset, row, 0.0)
        across_ref[t : t + 1, :] = row
    here = as_bf16(
        iota((z.rows, z.levels), 0) + part * z.rows == iota((z.rows, z.levels), 1)
    )
    down = jnp.zeros((z.rows, across_ref.shape[0]), F32)
    for values in thirds(across_ref[...]):
        down = down + dot_nt(here, values)
    for t in range(taps):
        spread[t] = jnp.broadcast_to(down[:, t : t + 1], (z.rows, LANES))
    tiles = z.levels // LANES
    mid_scr[...] = mid_ref[...]
    for g in range(z.slots):
        live = jnp.where(g < own, 1.0, 0.0)
        damp = damp_ref[g, 0:1, 0:1]
        fields = [mid_scr[g, c * z.rows : (c + 1) * z.rows, :] for c in range(2)]
        for c in range(2):
            field = fields[c]
            wide[0 : z.band, :] = low_ref[g, c]
            wide[z.band : z.band + z.rows, :] = field
            wide[z.band + z.rows :, :] = high_ref[g, c]
            summed = across_ref[z.band : z.band + 1, :] * field
            for t in range(taps):
                if t != z.band:
                    moved = pltpu.roll(field, (z.band - t) % z.levels, 1)
                    summed = summed + across_ref[t : t + 1, :] * moved
            sides = []
            for q in range(tiles):
                lanes = slice(q * LANES, (q + 1) * LANES)
                total = spread[0] * wide[0 : z.rows, lanes]
                for t in range(1, taps):
                    total = total + spread[t] * wide[t : t + z.rows, lanes]
                sides.append(total)
            commuted = jnp.concatenate(sides, axis=1) - summed
            other = 1 - c
            sign = 1.0 if c == 1 else -1.0
            out_ref[g, other * z.rows : (other + 1) * z.rows, :] = (
                live * (sign * commuted - damp * fields[other])
            )


def apply_kernel(
    z, got_ref, col_ref, row_ref, col_coef_ref, row_coef_ref, deriv_ref, base_ref,
    at_ref, sites_ref, next_ref, sum_ref, rows_scr, next_scr, sum_scr, sem,
):
    part = lax.axis_index("sys")
    at_site = jnp.concatenate([at_ref[...]] * 2, axis=0)
    total = z.slots * z.modes
    pieces = jnp.concatenate(
        [
            jnp.concatenate(
                [
                    got_ref[pl.ds(z.cap + j * z.lane_tiles + t, z.tiers, stride=z.message), :]
                    for t in range(z.lane_tiles)
                ],
                axis=1,
            )
            for j in range(z.row_cap)
        ],
        axis=0,
    )
    found = picked(row_ref[...].astype(BF16), pieces)
    half = z.slots * z.group
    up, down = found[:half], found[half:]
    real = jnp.concatenate([row_coef_ref[0, :, 0:1]] * z.slots, axis=0)
    imag = jnp.concatenate([row_coef_ref[1, :, 0:1]] * z.slots, axis=0)
    turned = up + real * down
    straight = imag * down
    rows_scr[0] = straight[:, : z.levels] + turned[:, z.levels :]
    rows_scr[1] = straight[:, z.levels :] - turned[:, : z.levels]
    pieces = jnp.concatenate(
        [got_ref[pl.ds(p, z.tiers, stride=z.message), :] for p in range(z.cap)], axis=0
    )
    found = picked(col_ref[...], pieces)
    sign = jnp.where(iota((1, 2 * z.rows), 1) < z.rows, -1.0, 1.0)
    for g in range(z.slots):
        up = found[g * z.modes : (g + 1) * z.modes]
        down = found[total + g * z.modes : total + (g + 1) * z.modes]
        cols = col_coef_ref[1] * down + sign * pltpu.roll(up + col_coef_ref[0] * down, z.rows, 1)
        added = dot_tn(jnp.concatenate(halves(cols), axis=0), at_site)
        next_scr[g] = deriv_ref[g] + added
        for k in range(z.block_modes):
            local = sites_ref[part * z.block_modes + k] - part * z.rows
            for c in range(2):
                at = pl.ds(c * z.rows + local, 1)
                row = g * z.group + k
                next_scr[g, at, :] = next_scr[g, at, :] + rows_scr[c, row : row + 1, :]
        pltpu.make_async_copy(next_scr.at[g], next_ref.at[g], sem.at[0, g]).start()
        sum_scr[g] = base_ref[g] + (step_size / 3.0) * next_scr[g]
        pltpu.make_async_copy(sum_scr.at[g], sum_ref.at[g], sem.at[1, g]).start()
    for g in range(z.slots):
        pltpu.make_async_copy(next_scr.at[g], next_ref.at[g], sem.at[0, g]).wait()
        pltpu.make_async_copy(sum_scr.at[g], sum_ref.at[g], sem.at[1, g]).wait()


def call(kernel, z, name, args, in_specs, outs, scratch=(), out_specs=None, micros=1, aliases=()):
    return pl.pallas_call(
        functools.partial(kernel, z),
        out_shape=outs,
        in_specs=in_specs,
        out_specs=[VMEM] * len(outs) if out_specs is None else out_specs,
        scratch_shapes=list(scratch),
        name=name,
        input_output_aliases=dict(aliases),
        compiler_params=pltpu.CompilerParams(vmem_limit_bytes=int(vmem_limits.get(name, 16) * mib)),
        cost_estimate=pl.CostEstimate(
            flops=int(micros * 1e6), bytes_accessed=int(micros * 1e5), transcendentals=0
        ),
    )(*args)


def neighbours(low_edge, high_edge):
    count = lax.axis_size("sys")
    forward = [(i, i + 1) for i in range(count - 1)]
    backward = [(target, source) for source, target in forward]
    return lax.ppermute(high_edge, "sys", forward), lax.ppermute(low_edge, "sys", backward)


def shards(state, slope, counts, links, mode_site, mode_coef, mode_rate, h_bands):
    z = Sizes(state, links, h_bands, lax.axis_size("tier"), lax.axis_size("sys"))
    shape = jax.ShapeDtypeStruct
    flat = (z.slots, 2 * z.rows, z.levels)
    state_flat = state.reshape(flat)
    slope_flat = slope.reshape(flat)
    (ask,) = call(
        ask_kernel, z, "ask", (links,), [VMEM], [shape((z.tiers, z.ask), jnp.int32)]
    )
    asked = lax.all_to_all(
        ask.reshape(z.tiers, 1, z.ask), "tier", split_axis=0, concat_axis=0, tiled=True
    ).reshape(z.tiers, z.ask)
    edge = (z.slots, 2, z.band, z.levels)
    low_edge, high_edge, col_table, row_table, mid, base = call(
        table_kernel,
        z,
        "tables",
        (state_flat, slope_flat, mode_site, counts),
        [VMEM, VMEM, SMEM, SMEM],
        [
            shape(edge, F32),
            shape(edge, F32),
            shape((3 * z.span, 2 * z.rows), BF16),
            shape((3 * z.row_pad, 2 * z.levels), BF16),
            shape(flat, F32),
            shape(flat, F32),
        ],
        [
            pltpu.VMEM((z.row_pad, 2 * z.levels), F32),
            pltpu.VMEM((round_up(z.modes, 16), z.levels), F32),
        ],
        micros=3,
    )
    (answer,) = call(
        answer_kernel,
        z,
        "answer",
        (asked, col_table, row_table),
        [VMEM] * 3,
        [shape((z.tiers * z.message, LANES), F32)],
    )
    got = lax.all_to_all(
        answer.reshape(z.tiers, 1, z.message * LANES),
        "tier",
        split_axis=0,
        concat_axis=0,
        tiled=True,
    ).reshape(z.tiers * z.message, LANES)
    low_edge, high_edge, answer_kept = lax.optimization_barrier((low_edge, high_edge, answer))
    above, below = neighbours(low_edge, high_edge)
    col_choice, row_choice, col_coef, row_coef, damp, at_site = call(
        choose_kernel,
        z,
        "choose",
        (links, counts[None], mode_coef, mode_rate[None], counts, mode_site),
        [VMEM] * 4 + [SMEM] * 2,
        [
            shape((2 * z.slots * z.modes, z.cap * z.tiers), BF16),
            shape((2 * z.slots * z.group, z.row_cap * z.tiers), F32),
            shape((2, z.modes, LANES), F32),
            shape((2, z.group, LANES), F32),
            shape((z.slots, 8, LANES), F32),
            shape((z.modes, z.levels), BF16),
        ],
        [pltpu.VMEM((round_up(z.modes, 16), z.levels), F32)],
        micros=2,
    )
    taps = round_up(2 * z.band + 1, 16)
    (deriv,) = call(
        band_kernel,
        z,
        "band",
        (mid, above, below, h_bands, damp, counts),
        [VMEM] * 5 + [SMEM],
        [shape(flat, F32)],
        [
            pltpu.VMEM((z.rows + 2 * z.band, z.levels), F32),
            pltpu.VMEM((2 * z.band + 1, z.rows, LANES), F32),
            pltpu.VMEM((taps, z.levels), F32),
            pltpu.VMEM(flat, F32),
        ],
        aliases=((0, 0),),
        micros=5,
    )
    slope_next, partial_sum = call(
        apply_kernel,
        z,
        "apply",
        (
            got, col_choice, row_choice, col_coef, row_coef, deriv, base, at_site, mode_site,
        ),
        [VMEM] * 8 + [SMEM],
        [shape(flat, F32), shape(flat, F32)],
        [
            pltpu.VMEM((2, z.slots * z.group, z.levels), F32),
            pltpu.VMEM(flat, F32),
            pltpu.VMEM(flat, F32),
            pltpu.SemaphoreType.DMA((2, z.slots)),
        ],
        out_specs=[HBM, HBM],
        micros=4,
    )
    return slope_next.reshape(state.shape), partial_sum.reshape(state.shape)


def solution(mesh):
    in_specs = (
        P("tier", None, "sys", None),
        P("tier", None, "sys", None),
        P(),
        P(None, "tier", None),
        P(),
        P(),
        P(),
        P(),
    )
    out_specs = (P("tier", None, "sys", None), P("tier", None, "sys", None))
    return jax.shard_map(shards, mesh=mesh, in_specs=in_specs, out_specs=out_specs, check_vma=False)
```

```python
import functools

import jax
import jax.numpy as jnp
from jax import lax
from jax.experimental import pallas as pl
from jax.experimental.pallas import tpu as pltpu
from jax.sharding import PartitionSpec as P

step_size = 0.05
LANES = 128
mib = 1024 * 1024
vmem_limits = {"ask": 61}
BF16 = jnp.bfloat16
F32 = jnp.float32
VMEM = pl.BlockSpec(memory_space=pltpu.VMEM)
SMEM = pl.BlockSpec(memory_space=pltpu.SMEM)
HBM = pl.BlockSpec(memory_space=pltpu.HBM)


def iota(shape, dim):
    return lax.broadcasted_iota(jnp.int32, shape, dim)


def round_up(value, multiple):
    return -(-value // multiple) * multiple


def dot_nn(a, b):
    return lax.dot_general(a, b, (((1,), (0,)), ((), ())), preferred_element_type=F32)


def dot_nt(a, b):
    return lax.dot_general(a, b, (((1,), (1,)), ((), ())), preferred_element_type=F32)


def dot_tn(a, b):
    return lax.dot_general(a, b, (((0,), (0,)), ((), ())), preferred_element_type=F32)


def thirds(x):
    first = x.astype(BF16)
    rest = x - first.astype(F32)
    second = rest.astype(BF16)
    third = (rest - second.astype(F32)).astype(BF16)
    return first, second, third


def halves(x):
    first = x.astype(BF16)
    return first, (x - first.astype(F32)).astype(BF16)


def picked(chooser, values):
    return dot_nn(
        jnp.concatenate([chooser, chooser], axis=1), jnp.concatenate(halves(values), axis=0)
    )


def as_bf16(mask):
    return jnp.where(mask, 1.0, 0.0).astype(BF16)


def as_column(row, size):
    diagonal = iota((size, size), 0) == iota((size, size), 1)
    return jnp.sum(jnp.where(diagonal, row, jnp.zeros((), row.dtype)), axis=1, keepdims=True)


class Sizes:
    def __init__(self, state, links, h_bands, tiers, parts):
        self.slots = state.shape[0]
        self.rows = state.shape[2]
        self.levels = state.shape[3]
        self.band = h_bands.shape[0] - 1
        self.per_slot = links.shape[2]
        self.tiers = tiers
        self.parts = parts
        self.modes = self.per_slot // 2
        self.block_modes = self.modes // parts
        total = self.slots * self.per_slot
        self.cap = total // tiers
        self.row_cap = 2 * ((self.slots * self.block_modes + tiers - 1) // tiers)
        self.lane_tiles = 2 * self.levels // LANES
        self.message = self.cap + self.row_cap * self.lane_tiles
        self.ask = round_up(2 * self.cap, 16)
        self.shift = self.slots.bit_length() - 1
        self.span = round_up(self.slots * self.modes, LANES)
        self.row_pad = round_up(self.slots * self.block_modes, 16)
        self.group = round_up(self.block_modes, 8)


def holders_of(z, links_ref, g):
    neighbour = links_ref[0, g : g + 1, :]
    holder = lax.shift_right_logical(neighbour, z.shift)
    target = lax.bitwise_and(neighbour, z.slots - 1)
    hit = holder == iota((z.tiers, z.per_slot), 0)
    return hit, holder, target


def earlier_table(size):
    return as_bf16(iota((size, size), 0) < iota((size, size), 1))


def rank_of(hit, seen, earlier):
    before = dot_nn(as_bf16(hit), earlier) + seen
    return jnp.sum(jnp.where(hit, before, 0.0), axis=0, keepdims=True).astype(jnp.int32)


def ask_kernel(z, links_ref, out_ref):
    earlier = earlier_table(z.per_slot)
    ones = jnp.ones((z.per_slot, z.per_slot), BF16)
    seen = jnp.zeros((z.tiers, z.per_slot), F32)
    table = jnp.zeros((z.tiers, z.ask), F32)
    field = iota((z.ask, z.per_slot), 0)
    for g in range(z.slots):
        hit, _, target = holders_of(z, links_ref, g)
        mode = links_ref[1, g : g + 1, :]
        rank = rank_of(hit, seen, earlier)
        value = jnp.where(lax.bitwise_and(field, 1) == 0, target, mode)
        value = jnp.where(lax.shift_right_logical(field, 1) == rank, value, 0)
        chosen = as_bf16(hit)
        table = table + dot_nt(chosen, value.astype(F32).astype(BF16))
        seen = seen + dot_nn(chosen, ones)
    out_ref[...] = table.astype(jnp.int32)


def table_kernel(
    z, state_ref, slope_ref, sites_ref, counts_ref, low_ref, high_ref, col_ref, row_ref, mid_ref,
    base_ref, rows_scr, site_scr,
):
    own = counts_ref[lax.axis_index("tier")]
    part = lax.axis_index("sys")
    lane = iota((1, z.levels), 1)
    used = z.slots * z.modes
    for third in range(3):
        if z.span > used:
            col_ref[third * z.span + used : (third + 1) * z.span, :] = jnp.zeros(
                (z.span - used, 2 * z.rows), BF16
            )
    for k in range(z.modes):
        site_scr[k : k + 1, :] = jnp.where(lane == sites_ref[k], 1.0, 0.0)
    at_site = site_scr[: z.modes, :].astype(BF16)
    rows_scr[...] = jnp.zeros_like(rows_scr)
    for g in range(z.slots):
        live = jnp.where(g < own, 1.0, 0.0)
        base_ref[g] = live * (state_ref[g] + (step_size / 6.0) * slope_ref[g])
        mid = state_ref[g] + (0.5 * step_size) * slope_ref[g]
        mid_ref[g] = mid
        for third, values in enumerate(thirds(mid)):
            at = third * z.span + g * z.modes
            col_ref[at : at + z.modes, :] = dot_nt(at_site, values).astype(BF16)
        for c in range(2):
            start = c * z.rows
            low_ref[g, c] = mid_ref[g, start : start + z.band, :]
            high_ref[g, c] = mid_ref[g, start + z.rows - z.band : start + z.rows, :]
            for k in range(z.block_modes):
                local = sites_ref[part * z.block_modes + k] - part * z.rows
                at = g * z.block_modes + k
                rows_scr[at : at + 1, c * z.levels : (c + 1) * z.levels] = mid_ref[
                    g, pl.ds(start + local, 1), :
                ]
    for third, values in enumerate(thirds(rows_scr[...])):
        row_ref[third * z.row_pad : (third + 1) * z.row_pad, :] = values


def answer_kernel(z, ask_ref, col_ref, row_ref, out_hbm, out_scr, sem):
    part = lax.axis_index("sys")
    low = part * z.block_modes
    asked = ask_ref[...]
    columns = []
    row_at = [jnp.full((z.tiers, 1), -1, jnp.int32) for _ in range(z.row_cap)]
    used = jnp.zeros((z.tiers, 1), jnp.int32)
    lanes = iota((z.tiers, z.span), 1)
    for p in range(z.cap):
        target = asked[:, 2 * p : 2 * p + 1]
        mode = asked[:, 2 * p + 1 : 2 * p + 2]
        columns.append(as_bf16(target * z.modes + mode == lanes))
        inside = jnp.logical_and(mode >= low, mode < low + z.block_modes)
        where_row = target * z.block_modes + (mode - low)
        for j in range(z.row_cap):
            take = jnp.logical_and(inside, used == j)
            row_at[j] = jnp.where(take, where_row, row_at[j])
        used = used + jnp.where(inside, 1, 0)
    lanes = iota((z.tiers, 3 * z.row_pad), 1)
    for third in (2, 1):
        lanes = jnp.where(lanes >= third * z.row_pad, lanes - third * z.row_pad, lanes)
    row_choice = [as_bf16(at == lanes) for at in row_at]
    pieces = 2
    size = z.tiers // pieces
    copies = []
    for piece in range(pieces):
        mine = slice(piece * size, (piece + 1) * size)
        start = piece * size * z.message
        found = dot_nn(jnp.concatenate([choice[mine] for choice in row_choice], axis=0), row_ref[...])
        for j in range(z.row_cap):
            for t in range(z.lane_tiles):
                at = start + z.cap + j * z.lane_tiles + t
                out_scr[pl.ds(at, size, stride=z.message), :] = found[
                    j * size : (j + 1) * size, t * LANES : (t + 1) * LANES
                ]
        chosen = jnp.concatenate([choice[mine] for choice in columns], axis=0)
        found = dot_nn(jnp.concatenate([chosen] * 3, axis=1), col_ref[...])
        for p in range(z.cap):
            out_scr[pl.ds(start + p, size, stride=z.message), :] = found[
                p * size : (p + 1) * size, :
            ]
        block = pl.ds(start, size * z.message)
        copies.append(
            pltpu.make_async_copy(out_scr.at[block], out_hbm.at[block], sem.at[piece])
        )
        copies[-1].start()
    for copy in copies:
        copy.wait()


def choose_kernel(
    z, links_ref, counts_ref, coef_ref, rate_ref, own_ref, sites_ref,
    col_ref, row_ref, col_coef_ref, row_coef_ref, damp_ref, at_ref, site_scr,
):
    part = lax.axis_index("sys")
    tier = lax.axis_index("tier")
    lane = iota((1, z.levels), 1)
    for k in range(z.modes):
        site_scr[k : k + 1, :] = jnp.where(lane == sites_ref[k], 1.0, 0.0)
    at_ref[...] = site_scr[: z.modes, :].astype(BF16)
    low = part * z.block_modes
    earlier = earlier_table(z.per_slot)
    ones = jnp.ones((z.per_slot, z.per_slot), BF16)
    seen = jnp.zeros((z.tiers, z.per_slot), F32)
    seen_rows = jnp.zeros((z.tiers, z.per_slot), F32)
    counts = as_column(counts_ref[...], z.tiers)
    rate = as_column(rate_ref[...], z.modes)
    coefs = [as_column(coef_ref[c : c + 1, :], z.modes) for c in range(2)]
    total = z.slots * z.modes
    for g in range(z.slots):
        hit, holder, target = holders_of(z, links_ref, g)
        mode = links_ref[1, g : g + 1, :]
        kind = links_ref[2, g : g + 1, :]
        level = links_ref[3, g : g + 1, :]
        rank = rank_of(hit, seen, earlier)
        seen = seen + dot_nn(as_bf16(hit), ones)
        inside = jnp.logical_and(mode >= low, mode < low + z.block_modes)
        hit_rows = jnp.logical_and(hit, inside)
        row_rank = rank_of(hit_rows, seen_rows, earlier)
        seen_rows = seen_rows + dot_nn(as_bf16(hit_rows), ones)
        live = target < jnp.sum(jnp.where(hit, counts, 0), axis=0, keepdims=True)
        live = jnp.logical_and(live, own_ref[tier] > g)
        scale = jnp.where(kind == 1, level, 1)
        here = as_bf16(iota((z.cap * z.tiers, z.per_slot), 0) == rank * z.tiers + holder)
        here_row = as_bf16(
            iota((z.row_cap * z.tiers, z.per_slot), 0) == row_rank * z.tiers + holder
        )
        modes = iota((z.modes, z.per_slot), 0)
        group = iota((z.group, z.per_slot), 0)
        for way in range(2):
            wanted = jnp.logical_and(kind == way, live)
            chosen = jnp.where(jnp.logical_and(modes == mode, wanted), scale, 0)
            at = way * total + g * z.modes
            col_ref[at : at + z.modes, :] = dot_nt(
                chosen.astype(F32).astype(BF16), here
            ).astype(BF16)
            own = jnp.logical_and(group + low == mode, jnp.logical_and(inside, wanted))
            at = (way * z.slots + g) * z.group
            row_ref[at : at + z.group, :] = dot_nt(
                jnp.where(own, scale, 0).astype(F32).astype(BF16), here_row
            )
        falling = jnp.where(jnp.logical_and(modes == mode, kind == 1), level, 0).astype(F32)
        amount = jnp.sum(falling, axis=1, keepdims=True) * rate
        damp_ref[g] = jnp.broadcast_to(jnp.sum(amount, axis=0, keepdims=True), (8, LANES))
    for c in range(2):
        col_coef_ref[c] = jnp.broadcast_to(coefs[c], (z.modes, LANES))
        mine = jnp.where(
            iota((z.group, z.modes), 0) + low == iota((z.group, z.modes), 1),
            coef_ref[c : c + 1, :],
            0.0,
        )
        mine = jnp.where(iota((z.group, z.modes), 0) < z.block_modes, mine, 0.0)
        row_coef_ref[c] = jnp.broadcast_to(
            jnp.sum(mine, axis=1, keepdims=True), (z.group, LANES)
        )


def band_kernel(
    z, mid_ref, low_ref, high_ref, bands_ref, damp_ref, counts_ref, out_ref, wide, spread,
    across_ref, mid_scr,
):
    part = lax.axis_index("sys")
    own = counts_ref[lax.axis_index("tier")]
    taps = 2 * z.band + 1
    across_ref[...] = jnp.zeros_like(across_ref)
    lane = iota((1, z.levels), 1)
    for t in range(taps):
        offset = t - z.band
        row = bands_ref[abs(offset) : abs(offset) + 1, :]
        if offset < 0:
            row = jnp.where(lane >= -offset, pltpu.roll(row, -offset, 1), 0.0)
        elif offset > 0:
            row = jnp.where(lane < z.levels - offset, row, 0.0)
        across_ref[t : t + 1, :] = row
    here = as_bf16(
        iota((z.rows, z.levels), 0) + part * z.rows == iota((z.rows, z.levels), 1)
    )
    down = jnp.zeros((z.rows, across_ref.shape[0]), F32)
    for values in thirds(across_ref[...]):
        down = down + dot_nt(here, values)
    for t in range(taps):
        spread[t] = jnp.broadcast_to(down[:, t : t + 1], (z.rows, LANES))
    tiles = z.levels // LANES
    mid_scr[...] = mid_ref[...]
    for g in range(z.slots):
        live = jnp.where(g < own, 1.0, 0.0)
        damp = damp_ref[g, 0:1, 0:1]
        fields = [mid_scr[g, c * z.rows : (c + 1) * z.rows, :] for c in range(2)]
        for c in range(2):
            field = fields[c]
            wide[0 : z.band, :] = low_ref[g, c]
            wide[z.band : z.band + z.rows, :] = field
            wide[z.band + z.rows :, :] = high_ref[g, c]
            summed = across_ref[z.band : z.band + 1, :] * field
            for t in range(taps):
                if t != z.band:
                    moved = pltpu.roll(field, (z.band - t) % z.levels, 1)
                    summed = summed + across_ref[t : t + 1, :] * moved
            sides = []
            for q in range(tiles):
                lanes = slice(q * LANES, (q + 1) * LANES)
                total = spread[0] * wide[0 : z.rows, lanes]
                for t in range(1, taps):
                    total = total + spread[t] * wide[t : t + z.rows, lanes]
                sides.append(total)
            commuted = jnp.concatenate(sides, axis=1) - summed
            other = 1 - c
            sign = 1.0 if c == 1 else -1.0
            out_ref[g, other * z.rows : (other + 1) * z.rows, :] = (
                live * (sign * commuted - damp * fields[other])
            )


def apply_kernel(
    z, got_ref, col_ref, row_ref, col_coef_ref, row_coef_ref, deriv_ref, base_ref,
    at_ref, sites_ref, next_ref, sum_ref, rows_scr, next_scr, sum_scr, sem,
):
    part = lax.axis_index("sys")
    at_site = jnp.concatenate([at_ref[...]] * 2, axis=0)
    total = z.slots * z.modes
    pieces = jnp.concatenate(
        [
            jnp.concatenate(
                [
                    got_ref[pl.ds(z.cap + j * z.lane_tiles + t, z.tiers, stride=z.message), :]
                    for t in range(z.lane_tiles)
                ],
                axis=1,
            )
            for j in range(z.row_cap)
        ],
        axis=0,
    )
    found = picked(row_ref[...].astype(BF16), pieces)
    half = z.slots * z.group
    up, down = found[:half], found[half:]
    real = jnp.concatenate([row_coef_ref[0, :, 0:1]] * z.slots, axis=0)
    imag = jnp.concatenate([row_coef_ref[1, :, 0:1]] * z.slots, axis=0)
    turned = up + real * down
    straight = imag * down
    rows_scr[0] = straight[:, : z.levels] + turned[:, z.levels :]
    rows_scr[1] = straight[:, z.levels :] - turned[:, : z.levels]
    pieces = jnp.concatenate(
        [got_ref[pl.ds(p, z.tiers, stride=z.message), :] for p in range(z.cap)], axis=0
    )
    found = picked(col_ref[...], pieces)
    sign = jnp.where(iota((1, 2 * z.rows), 1) < z.rows, -1.0, 1.0)
    for g in range(z.slots):
        up = found[g * z.modes : (g + 1) * z.modes]
        down = found[total + g * z.modes : total + (g + 1) * z.modes]
        cols = col_coef_ref[1] * down + sign * pltpu.roll(up + col_coef_ref[0] * down, z.rows, 1)
        added = dot_tn(jnp.concatenate(halves(cols), axis=0), at_site)
        next_scr[g] = deriv_ref[g] + added
        for k in range(z.block_modes):
            local = sites_ref[part * z.block_modes + k] - part * z.rows
            for c in range(2):
                at = pl.ds(c * z.rows + local, 1)
                row = g * z.group + k
                next_scr[g, at, :] = next_scr[g, at, :] + rows_scr[c, row : row + 1, :]
        pltpu.make_async_copy(next_scr.at[g], next_ref.at[g], sem.at[0, g]).start()
        sum_scr[g] = base_ref[g] + (step_size / 3.0) * next_scr[g]
        pltpu.make_async_copy(sum_scr.at[g], sum_ref.at[g], sem.at[1, g]).start()
    for g in range(z.slots):
        pltpu.make_async_copy(next_scr.at[g], next_ref.at[g], sem.at[0, g]).wait()
        pltpu.make_async_copy(sum_scr.at[g], sum_ref.at[g], sem.at[1, g]).wait()


def call(kernel, z, name, args, in_specs, outs, scratch=(), out_specs=None, micros=1, aliases=()):
    return pl.pallas_call(
        functools.partial(kernel, z),
        out_shape=outs,
        in_specs=in_specs,
        out_specs=[VMEM] * len(outs) if out_specs is None else out_specs,
        scratch_shapes=list(scratch),
        name=name,
        input_output_aliases=dict(aliases),
        compiler_params=pltpu.CompilerParams(vmem_limit_bytes=int(vmem_limits.get(name, 16) * mib)),
        cost_estimate=pl.CostEstimate(
            flops=int(micros * 1e6), bytes_accessed=int(micros * 1e5), transcendentals=0
        ),
    )(*args)


def neighbours(low_edge, high_edge):
    count = lax.axis_size("sys")
    forward = [(i, i + 1) for i in range(count - 1)]
    backward = [(target, source) for source, target in forward]
    return lax.ppermute(high_edge, "sys", forward), lax.ppermute(low_edge, "sys", backward)


def shards(state, slope, counts, links, mode_site, mode_coef, mode_rate, h_bands):
    z = Sizes(state, links, h_bands, lax.axis_size("tier"), lax.axis_size("sys"))
    shape = jax.ShapeDtypeStruct
    flat = (z.slots, 2 * z.rows, z.levels)
    state_flat = state.reshape(flat)
    slope_flat = slope.reshape(flat)
    (ask,) = call(
        ask_kernel, z, "ask", (links,), [VMEM], [shape((z.tiers, z.ask), jnp.int32)]
    )
    asked = lax.all_to_all(
        ask.reshape(z.tiers, 1, z.ask), "tier", split_axis=0, concat_axis=0, tiled=True
    ).reshape(z.tiers, z.ask)
    edge = (z.slots, 2, z.band, z.levels)
    low_edge, high_edge, col_table, row_table, mid, base = call(
        table_kernel,
        z,
        "tables",
        (state_flat, slope_flat, mode_site, counts),
        [VMEM, VMEM, SMEM, SMEM],
        [
            shape(edge, F32),
            shape(edge, F32),
            shape((3 * z.span, 2 * z.rows), BF16),
            shape((3 * z.row_pad, 2 * z.levels), BF16),
            shape(flat, F32),
            shape(flat, F32),
        ],
        [
            pltpu.VMEM((z.row_pad, 2 * z.levels), F32),
            pltpu.VMEM((round_up(z.modes, 16), z.levels), F32),
        ],
        micros=3,
    )
    (answer,) = call(
        answer_kernel,
        z,
        "answer",
        (asked, col_table, row_table),
        [VMEM] * 3,
        [shape((z.tiers * z.message, LANES), F32)],
        [pltpu.VMEM((z.tiers * z.message, LANES), F32), pltpu.SemaphoreType.DMA((2,))],
        out_specs=[HBM],
    )
    got = lax.all_to_all(
        answer.reshape(z.tiers, 1, z.message * LANES),
        "tier",
        split_axis=0,
        concat_axis=0,
        tiled=True,
    ).reshape(z.tiers * z.message, LANES)
    low_edge, high_edge, answer_kept = lax.optimization_barrier((low_edge, high_edge, answer))
    above, below = neighbours(low_edge, high_edge)
    col_choice, row_choice, col_coef, row_coef, damp, at_site = call(
        choose_kernel,
        z,
        "choose",
        (links, counts[None], mode_coef, mode_rate[None], counts, mode_site),
        [VMEM] * 4 + [SMEM] * 2,
        [
            shape((2 * z.slots * z.modes, z.cap * z.tiers), BF16),
            shape((2 * z.slots * z.group, z.row_cap * z.tiers), F32),
            shape((2, z.modes, LANES), F32),
            shape((2, z.group, LANES), F32),
            shape((z.slots, 8, LANES), F32),
            shape((z.modes, z.levels), BF16),
        ],
        [pltpu.VMEM((round_up(z.modes, 16), z.levels), F32)],
        micros=2,
    )
    taps = round_up(2 * z.band + 1, 16)
    (deriv,) = call(
        band_kernel,
        z,
        "band",
        (mid, above, below, h_bands, damp, counts),
        [VMEM] * 5 + [SMEM],
        [shape(flat, F32)],
        [
            pltpu.VMEM((z.rows + 2 * z.band, z.levels), F32),
            pltpu.VMEM((2 * z.band + 1, z.rows, LANES), F32),
            pltpu.VMEM((taps, z.levels), F32),
            pltpu.VMEM(flat, F32),
        ],
        aliases=((0, 0),),
        micros=5,
    )
    slope_next, partial_sum = call(
        apply_kernel,
        z,
        "apply",
        (
            got, col_choice, row_choice, col_coef, row_coef, deriv, base, at_site, mode_site,
        ),
        [VMEM] * 8 + [SMEM],
        [shape(flat, F32), shape(flat, F32)],
        [
            pltpu.VMEM((2, z.slots * z.group, z.levels), F32),
            pltpu.VMEM(flat, F32),
            pltpu.VMEM(flat, F32),
            pltpu.SemaphoreType.DMA((2, z.slots)),
        ],
        out_specs=[HBM, HBM],
        micros=4,
    )
    return slope_next.reshape(state.shape), partial_sum.reshape(state.shape)


def solution(mesh):
    in_specs = (
        P("tier", None, "sys", None),
        P("tier", None, "sys", None),
        P(),
        P(None, "tier", None),
        P(),
        P(),
        P(),
        P(),
    )
    out_specs = (P("tier", None, "sys", None), P("tier", None, "sys", None))
    return jax.shard_map(shards, mesh=mesh, in_specs=in_specs, out_specs=out_specs, check_vma=False)
```

```python
import functools

import jax
import jax.numpy as jnp
from jax import lax
from jax.experimental import pallas as pl
from jax.experimental.pallas import tpu as pltpu
from jax.sharding import PartitionSpec as P

step_size = 0.05
LANES = 128
mib = 1024 * 1024
vmem_limits = {"tables": 16, "band": 16, "apply": 16}
BF16 = jnp.bfloat16
F32 = jnp.float32
VMEM = pl.BlockSpec(memory_space=pltpu.VMEM)
SMEM = pl.BlockSpec(memory_space=pltpu.SMEM)
HBM = pl.BlockSpec(memory_space=pltpu.HBM)


def iota(shape, dim):
    return lax.broadcasted_iota(jnp.int32, shape, dim)


def round_up(value, multiple):
    return -(-value // multiple) * multiple


def dot_nn(a, b):
    return lax.dot_general(a, b, (((1,), (0,)), ((), ())), preferred_element_type=F32)


def dot_nt(a, b):
    return lax.dot_general(a, b, (((1,), (1,)), ((), ())), preferred_element_type=F32)


def dot_tn(a, b):
    return lax.dot_general(a, b, (((0,), (0,)), ((), ())), preferred_element_type=F32)


def thirds(x):
    first = x.astype(BF16)
    rest = x - first.astype(F32)
    second = rest.astype(BF16)
    third = (rest - second.astype(F32)).astype(BF16)
    return first, second, third


def halves(x):
    first = x.astype(BF16)
    return first, (x - first.astype(F32)).astype(BF16)


def picked(chooser, values):
    return dot_nn(
        jnp.concatenate([chooser, chooser], axis=1), jnp.concatenate(halves(values), axis=0)
    )


def as_bf16(mask):
    return jnp.where(mask, 1.0, 0.0).astype(BF16)


def as_column(row, size):
    diagonal = iota((size, size), 0) == iota((size, size), 1)
    return jnp.sum(jnp.where(diagonal, row, jnp.zeros((), row.dtype)), axis=1, keepdims=True)


class Sizes:
    def __init__(self, state, links, h_bands, tiers, parts):
        self.slots = state.shape[0]
        self.rows = state.shape[2]
        self.levels = state.shape[3]
        self.band = h_bands.shape[0] - 1
        self.per_slot = links.shape[2]
        self.tiers = tiers
        self.parts = parts
        self.modes = self.per_slot // 2
        self.block_modes = self.modes // parts
        total = self.slots * self.per_slot
        self.cap = total // tiers
        self.row_cap = 2 * ((self.slots * self.block_modes + tiers - 1) // tiers)
        self.lane_tiles = 2 * self.levels // LANES
        self.message = self.cap + self.row_cap * self.lane_tiles
        self.ask = round_up(2 * self.cap, 16)
        self.shift = self.slots.bit_length() - 1
        self.span = round_up(self.slots * self.modes, LANES)
        self.row_pad = round_up(self.slots * self.block_modes, 16)
        self.group = round_up(self.block_modes, 8)


def holders_of(z, links_ref, g):
    neighbour = links_ref[0, g : g + 1, :]
    holder = lax.shift_right_logical(neighbour, z.shift)
    target = lax.bitwise_and(neighbour, z.slots - 1)
    hit = holder == iota((z.tiers, z.per_slot), 0)
    return hit, holder, target


def earlier_table(size):
    return as_bf16(iota((size, size), 0) < iota((size, size), 1))


def rank_of(hit, seen, earlier):
    before = dot_nn(as_bf16(hit), earlier) + seen
    return jnp.sum(jnp.where(hit, before, 0.0), axis=0, keepdims=True).astype(jnp.int32)


def ask_kernel(z, links_ref, out_ref):
    earlier = earlier_table(z.per_slot)
    ones = jnp.ones((z.per_slot, z.per_slot), BF16)
    seen = jnp.zeros((z.tiers, z.per_slot), F32)
    table = jnp.zeros((z.tiers, z.ask), F32)
    field = iota((z.ask, z.per_slot), 0)
    for g in range(z.slots):
        hit, _, target = holders_of(z, links_ref, g)
        mode = links_ref[1, g : g + 1, :]
        rank = rank_of(hit, seen, earlier)
        value = jnp.where(lax.bitwise_and(field, 1) == 0, target, mode)
        value = jnp.where(lax.shift_right_logical(field, 1) == rank, value, 0)
        chosen = as_bf16(hit)
        table = table + dot_nt(chosen, value.astype(F32).astype(BF16))
        seen = seen + dot_nn(chosen, ones)
    out_ref[...] = table.astype(jnp.int32)


def table_kernel(
    z, state_ref, slope_ref, sites_ref, counts_ref, low_ref, high_ref, col_ref, row_ref, mid_ref,
    base_ref, rows_scr, site_scr,
):
    own = counts_ref[lax.axis_index("tier")]
    part = lax.axis_index("sys")
    lane = iota((1, z.levels), 1)
    used = z.slots * z.modes
    for third in range(3):
        if z.span > used:
            col_ref[third * z.span + used : (third + 1) * z.span, :] = jnp.zeros(
                (z.span - used, 2 * z.rows), BF16
            )
    for k in range(z.modes):
        site_scr[k : k + 1, :] = jnp.where(lane == sites_ref[k], 1.0, 0.0)
    at_site = site_scr[: z.modes, :].astype(BF16)
    rows_scr[...] = jnp.zeros_like(rows_scr)
    for g in range(z.slots):
        live = jnp.where(g < own, 1.0, 0.0)
        base_ref[g] = live * (state_ref[g] + (step_size / 6.0) * slope_ref[g])
        mid = state_ref[g] + (0.5 * step_size) * slope_ref[g]
        mid_ref[g] = mid
        for third, values in enumerate(thirds(mid)):
            at = third * z.span + g * z.modes
            col_ref[at : at + z.modes, :] = dot_nt(at_site, values).astype(BF16)
        for c in range(2):
            start = c * z.rows
            low_ref[g, c] = mid_ref[g, start : start + z.band, :]
            high_ref[g, c] = mid_ref[g, start + z.rows - z.band : start + z.rows, :]
            for k in range(z.block_modes):
                local = sites_ref[part * z.block_modes + k] - part * z.rows
                at = g * z.block_modes + k
                rows_scr[at : at + 1, c * z.levels : (c + 1) * z.levels] = mid_ref[
                    g, pl.ds(start + local, 1), :
                ]
    for third, values in enumerate(thirds(rows_scr[...])):
        row_ref[third * z.row_pad : (third + 1) * z.row_pad, :] = values


def answer_kernel(z, ask_ref, col_ref, row_ref, out_ref):
    part = lax.axis_index("sys")
    low = part * z.block_modes
    asked = ask_ref[...]
    columns = []
    row_at = [jnp.full((z.tiers, 1), -1, jnp.int32) for _ in range(z.row_cap)]
    used = jnp.zeros((z.tiers, 1), jnp.int32)
    lanes = iota((z.tiers, z.span), 1)
    for p in range(z.cap):
        target = asked[:, 2 * p : 2 * p + 1]
        mode = asked[:, 2 * p + 1 : 2 * p + 2]
        columns.append(as_bf16(target * z.modes + mode == lanes))
        inside = jnp.logical_and(mode >= low, mode < low + z.block_modes)
        where_row = target * z.block_modes + (mode - low)
        for j in range(z.row_cap):
            take = jnp.logical_and(inside, used == j)
            row_at[j] = jnp.where(take, where_row, row_at[j])
        used = used + jnp.where(inside, 1, 0)
    lanes = iota((z.tiers, 3 * z.row_pad), 1)
    for third in (2, 1):
        lanes = jnp.where(lanes >= third * z.row_pad, lanes - third * z.row_pad, lanes)
    chosen = jnp.concatenate([as_bf16(at == lanes) for at in row_at], axis=0)
    found = dot_nn(chosen, row_ref[...])
    for j in range(z.row_cap):
        for t in range(z.lane_tiles):
            at = z.cap + j * z.lane_tiles + t
            out_ref[pl.ds(at, z.tiers, stride=z.message), :] = found[
                j * z.tiers : (j + 1) * z.tiers, t * LANES : (t + 1) * LANES
            ]
    chosen = jnp.concatenate(columns, axis=0)
    found = dot_nn(jnp.concatenate([chosen] * 3, axis=1), col_ref[...])
    for p in range(z.cap):
        out_ref[pl.ds(p, z.tiers, stride=z.message), :] = found[p * z.tiers : (p + 1) * z.tiers, :]


def choose_kernel(
    z, links_ref, counts_ref, coef_ref, rate_ref, own_ref, sites_ref,
    col_ref, row_ref, col_coef_ref, row_coef_ref, damp_ref, at_ref, site_scr,
):
    part = lax.axis_index("sys")
    tier = lax.axis_index("tier")
    lane = iota((1, z.levels), 1)
    for k in range(z.modes):
        site_scr[k : k + 1, :] = jnp.where(lane == sites_ref[k], 1.0, 0.0)
    at_ref[...] = site_scr[: z.modes, :].astype(BF16)
    low = part * z.block_modes
    earlier = earlier_table(z.per_slot)
    ones = jnp.ones((z.per_slot, z.per_slot), BF16)
    seen = jnp.zeros((z.tiers, z.per_slot), F32)
    seen_rows = jnp.zeros((z.tiers, z.per_slot), F32)
    counts = as_column(counts_ref[...], z.tiers)
    rate = as_column(rate_ref[...], z.modes)
    coefs = [as_column(coef_ref[c : c + 1, :], z.modes) for c in range(2)]
    total = z.slots * z.modes
    for g in range(z.slots):
        hit, holder, target = holders_of(z, links_ref, g)
        mode = links_ref[1, g : g + 1, :]
        kind = links_ref[2, g : g + 1, :]
        level = links_ref[3, g : g + 1, :]
        rank = rank_of(hit, seen, earlier)
        seen = seen + dot_nn(as_bf16(hit), ones)
        inside = jnp.logical_and(mode >= low, mode < low + z.block_modes)
        hit_rows = jnp.logical_and(hit, inside)
        row_rank = rank_of(hit_rows, seen_rows, earlier)
        seen_rows = seen_rows + dot_nn(as_bf16(hit_rows), ones)
        live = target < jnp.sum(jnp.where(hit, counts, 0), axis=0, keepdims=True)
        live = jnp.logical_and(live, own_ref[tier] > g)
        scale = jnp.where(kind == 1, level, 1)
        here = as_bf16(iota((z.cap * z.tiers, z.per_slot), 0) == rank * z.tiers + holder)
        here_row = as_bf16(
            iota((z.row_cap * z.tiers, z.per_slot), 0) == row_rank * z.tiers + holder
        )
        modes = iota((z.modes, z.per_slot), 0)
        group = iota((z.group, z.per_slot), 0)
        for way in range(2):
            wanted = jnp.logical_and(kind == way, live)
            chosen = jnp.where(jnp.logical_and(modes == mode, wanted), scale, 0)
            at = way * total + g * z.modes
            col_ref[at : at + z.modes, :] = dot_nt(
                chosen.astype(F32).astype(BF16), here
            ).astype(BF16)
            own = jnp.logical_and(group + low == mode, jnp.logical_and(inside, wanted))
            at = (way * z.slots + g) * z.group
            row_ref[at : at + z.group, :] = dot_nt(
                jnp.where(own, scale, 0).astype(F32).astype(BF16), here_row
            )
        falling = jnp.where(jnp.logical_and(modes == mode, kind == 1), level, 0).astype(F32)
        amount = jnp.sum(falling, axis=1, keepdims=True) * rate
        damp_ref[g] = jnp.broadcast_to(jnp.sum(amount, axis=0, keepdims=True), (8, LANES))
    for c in range(2):
        col_coef_ref[c] = jnp.broadcast_to(coefs[c], (z.modes, LANES))
        mine = jnp.where(
            iota((z.group, z.modes), 0) + low == iota((z.group, z.modes), 1),
            coef_ref[c : c + 1, :],
            0.0,
        )
        mine = jnp.where(iota((z.group, z.modes), 0) < z.block_modes, mine, 0.0)
        row_coef_ref[c] = jnp.broadcast_to(
            jnp.sum(mine, axis=1, keepdims=True), (z.group, LANES)
        )


def band_kernel(
    z, mid_ref, low_ref, high_ref, bands_ref, damp_ref, counts_ref, out_ref, wide, spread,
    across_ref, mid_scr,
):
    part = lax.axis_index("sys")
    own = counts_ref[lax.axis_index("tier")]
    taps = 2 * z.band + 1
    across_ref[...] = jnp.zeros_like(across_ref)
    lane = iota((1, z.levels), 1)
    for t in range(taps):
        offset = t - z.band
        row = bands_ref[abs(offset) : abs(offset) + 1, :]
        if offset < 0:
            row = jnp.where(lane >= -offset, pltpu.roll(row, -offset, 1), 0.0)
        elif offset > 0:
            row = jnp.where(lane < z.levels - offset, row, 0.0)
        across_ref[t : t + 1, :] = row
    here = as_bf16(
        iota((z.rows, z.levels), 0) + part * z.rows == iota((z.rows, z.levels), 1)
    )
    down = jnp.zeros((z.rows, across_ref.shape[0]), F32)
    for values in thirds(across_ref[...]):
        down = down + dot_nt(here, values)
    for t in range(taps):
        spread[t] = jnp.broadcast_to(down[:, t : t + 1], (z.rows, LANES))
    tiles = z.levels // LANES
    mid_scr[...] = mid_ref[...]
    for g in range(z.slots):
        live = jnp.where(g < own, 1.0, 0.0)
        damp = damp_ref[g, 0:1, 0:1]
        fields = [mid_scr[g, c * z.rows : (c + 1) * z.rows, :] for c in range(2)]
        for c in range(2):
            field = fields[c]
            wide[0 : z.band, :] = low_ref[g, c]
            wide[z.band : z.band + z.rows, :] = field
            wide[z.band + z.rows :, :] = high_ref[g, c]
            summed = across_ref[z.band : z.band + 1, :] * field
            for t in range(taps):
                if t != z.band:
                    moved = pltpu.roll(field, (z.band - t) % z.levels, 1)
                    summed = summed + across_ref[t : t + 1, :] * moved
            sides = []
            for q in range(tiles):
                lanes = slice(q * LANES, (q + 1) * LANES)
                total = spread[0] * wide[0 : z.rows, lanes]
                for t in range(1, taps):
                    total = total + spread[t] * wide[t : t + z.rows, lanes]
                sides.append(total)
            commuted = jnp.concatenate(sides, axis=1) - summed
            other = 1 - c
            sign = 1.0 if c == 1 else -1.0
            out_ref[g, other * z.rows : (other + 1) * z.rows, :] = (
                live * (sign * commuted - damp * fields[other])
            )


def apply_kernel(
    z, got_ref, col_ref, row_ref, col_coef_ref, row_coef_ref, deriv_ref, base_ref,
    at_ref, sites_ref, next_ref, sum_ref, next_scr, sum_scr, sem,
):
    part = lax.axis_index("sys")
    at_site = jnp.concatenate([at_ref[...]] * 2, axis=0)
    total = z.slots * z.modes
    pieces = jnp.concatenate(
        [
            jnp.concatenate(
                [
                    got_ref[pl.ds(z.cap + j * z.lane_tiles + t, z.tiers, stride=z.message), :]
                    for t in range(z.lane_tiles)
                ],
                axis=1,
            )
            for j in range(z.row_cap)
        ],
        axis=0,
    )
    found = picked(row_ref[...].astype(BF16), pieces)
    half = z.slots * z.group
    up, down = found[:half], found[half:]
    real = jnp.concatenate([row_coef_ref[0, :, 0:1]] * z.slots, axis=0)
    imag = jnp.concatenate([row_coef_ref[1, :, 0:1]] * z.slots, axis=0)
    turned = up + real * down
    straight = imag * down
    real_rows = straight[:, : z.levels] + turned[:, z.levels :]
    imag_rows = straight[:, z.levels :] - turned[:, : z.levels]
    target = jnp.full((2 * z.group, 2 * z.rows), -1, jnp.int32)
    line = iota((2 * z.group, 2 * z.rows), 0)
    for k in range(z.block_modes):
        local = sites_ref[part * z.block_modes + k] - part * z.rows
        for c in range(2):
            target = jnp.where(line == c * z.group + k, c * z.rows + local, target)
    at_row = as_bf16(iota((2 * z.group, 2 * z.rows), 1) == target)
    pieces = jnp.concatenate(
        [got_ref[pl.ds(p, z.tiers, stride=z.message), :] for p in range(z.cap)], axis=0
    )
    found = picked(col_ref[...], pieces)
    sign = jnp.where(iota((1, 2 * z.rows), 1) < z.rows, -1.0, 1.0)
    for g in range(z.slots):
        up = found[g * z.modes : (g + 1) * z.modes]
        down = found[total + g * z.modes : total + (g + 1) * z.modes]
        cols = col_coef_ref[1] * down + sign * pltpu.roll(up + col_coef_ref[0] * down, z.rows, 1)
        mine = slice(g * z.group, (g + 1) * z.group)
        own = halves(jnp.concatenate([real_rows[mine], imag_rows[mine]], axis=0))
        slope_next = deriv_ref[g] + dot_tn(
            jnp.concatenate([*halves(cols), at_row, at_row], axis=0),
            jnp.concatenate([at_site, *own], axis=0),
        )
        next_scr[g] = slope_next
        pltpu.make_async_copy(next_scr.at[g], next_ref.at[g], sem.at[0, g]).start()
        sum_scr[g] = base_ref[g] + (step_size / 3.0) * slope_next
        pltpu.make_async_copy(sum_scr.at[g], sum_ref.at[g], sem.at[1, g]).start()
    for g in range(z.slots):
        pltpu.make_async_copy(next_scr.at[g], next_ref.at[g], sem.at[0, g]).wait()
        pltpu.make_async_copy(sum_scr.at[g], sum_ref.at[g], sem.at[1, g]).wait()


def call(kernel, z, name, args, in_specs, outs, scratch=(), out_specs=None, micros=1, aliases=()):
    return pl.pallas_call(
        functools.partial(kernel, z),
        out_shape=outs,
        in_specs=in_specs,
        out_specs=[VMEM] * len(outs) if out_specs is None else out_specs,
        scratch_shapes=list(scratch),
        name=name,
        input_output_aliases=dict(aliases),
        compiler_params=pltpu.CompilerParams(vmem_limit_bytes=int(vmem_limits.get(name, 16) * mib)),
        cost_estimate=pl.CostEstimate(
            flops=int(micros * 1e6), bytes_accessed=int(micros * 1e5), transcendentals=0
        ),
    )(*args)


def neighbours(low_edge, high_edge):
    count = lax.axis_size("sys")
    forward = [(i, i + 1) for i in range(count - 1)]
    backward = [(target, source) for source, target in forward]
    return lax.ppermute(high_edge, "sys", forward), lax.ppermute(low_edge, "sys", backward)


def shards(state, slope, counts, links, mode_site, mode_coef, mode_rate, h_bands):
    z = Sizes(state, links, h_bands, lax.axis_size("tier"), lax.axis_size("sys"))
    shape = jax.ShapeDtypeStruct
    flat = (z.slots, 2 * z.rows, z.levels)
    state_flat = state.reshape(flat)
    slope_flat = slope.reshape(flat)
    (ask,) = call(
        ask_kernel, z, "ask", (links,), [VMEM], [shape((z.tiers, z.ask), jnp.int32)]
    )
    asked = lax.all_to_all(
        ask.reshape(z.tiers, 1, z.ask), "tier", split_axis=0, concat_axis=0, tiled=True
    ).reshape(z.tiers, z.ask)
    edge = (z.slots, 2, z.band, z.levels)
    low_edge, high_edge, col_table, row_table, mid, base = call(
        table_kernel,
        z,
        "tables",
        (state_flat, slope_flat, mode_site, counts),
        [VMEM, VMEM, SMEM, SMEM],
        [
            shape(edge, F32),
            shape(edge, F32),
            shape((3 * z.span, 2 * z.rows), BF16),
            shape((3 * z.row_pad, 2 * z.levels), BF16),
            shape(flat, F32),
            shape(flat, F32),
        ],
        [
            pltpu.VMEM((z.row_pad, 2 * z.levels), F32),
            pltpu.VMEM((round_up(z.modes, 16), z.levels), F32),
        ],
        micros=3,
    )
    (answer,) = call(
        answer_kernel,
        z,
        "answer",
        (asked, col_table, row_table),
        [VMEM] * 3,
        [shape((z.tiers * z.message, LANES), F32)],
    )
    got = lax.all_to_all(
        answer.reshape(z.tiers, 1, z.message * LANES),
        "tier",
        split_axis=0,
        concat_axis=0,
        tiled=True,
    ).reshape(z.tiers * z.message, LANES)
    low_edge, high_edge, answer_kept = lax.optimization_barrier((low_edge, high_edge, answer))
    above, below = neighbours(low_edge, high_edge)
    col_choice, row_choice, col_coef, row_coef, damp, at_site = call(
        choose_kernel,
        z,
        "choose",
        (links, counts[None], mode_coef, mode_rate[None], counts, mode_site),
        [VMEM] * 4 + [SMEM] * 2,
        [
            shape((2 * z.slots * z.modes, z.cap * z.tiers), BF16),
            shape((2 * z.slots * z.group, z.row_cap * z.tiers), F32),
            shape((2, z.modes, LANES), F32),
            shape((2, z.group, LANES), F32),
            shape((z.slots, 8, LANES), F32),
            shape((z.modes, z.levels), BF16),
        ],
        [pltpu.VMEM((round_up(z.modes, 16), z.levels), F32)],
        micros=2,
    )
    taps = round_up(2 * z.band + 1, 16)
    (deriv,) = call(
        band_kernel,
        z,
        "band",
        (mid, above, below, h_bands, damp, counts),
        [VMEM] * 5 + [SMEM],
        [shape(flat, F32)],
        [
            pltpu.VMEM((z.rows + 2 * z.band, z.levels), F32),
            pltpu.VMEM((2 * z.band + 1, z.rows, LANES), F32),
            pltpu.VMEM((taps, z.levels), F32),
            pltpu.VMEM(flat, F32),
        ],
        aliases=((0, 0),),
        micros=5,
    )
    slope_next, partial_sum = call(
        apply_kernel,
        z,
        "apply",
        (
            got, col_choice, row_choice, col_coef, row_coef, deriv, base, at_site, mode_site,
        ),
        [VMEM] * 8 + [SMEM],
        [shape(flat, F32), shape(flat, F32)],
        [
            pltpu.VMEM(flat, F32),
            pltpu.VMEM(flat, F32),
            pltpu.SemaphoreType.DMA((2, z.slots)),
        ],
        out_specs=[HBM, HBM],
        micros=4,
    )
    return slope_next.reshape(state.shape), partial_sum.reshape(state.shape)


def solution(mesh):
    in_specs = (
        P("tier", None, "sys", None),
        P("tier", None, "sys", None),
        P(),
        P(None, "tier", None),
        P(),
        P(),
        P(),
        P(),
    )
    out_specs = (P("tier", None, "sys", None), P("tier", None, "sys", None))
    return jax.shard_map(shards, mesh=mesh, in_specs=in_specs, out_specs=out_specs, check_vma=False)
```

```python
import functools

import jax
import jax.numpy as jnp
from jax import lax
from jax.experimental import pallas as pl
from jax.experimental.pallas import tpu as pltpu
from jax.sharding import PartitionSpec as P

step_size = 0.05
LANES = 128
mib = 1024 * 1024
vmem_limits = {"tables": 16, "band": 16, "apply": 16}
BF16 = jnp.bfloat16
F32 = jnp.float32
VMEM = pl.BlockSpec(memory_space=pltpu.VMEM)
SMEM = pl.BlockSpec(memory_space=pltpu.SMEM)
HBM = pl.BlockSpec(memory_space=pltpu.HBM)


def iota(shape, dim):
    return lax.broadcasted_iota(jnp.int32, shape, dim)


def round_up(value, multiple):
    return -(-value // multiple) * multiple


def dot_nn(a, b):
    return lax.dot_general(a, b, (((1,), (0,)), ((), ())), preferred_element_type=F32)


def dot_nt(a, b):
    return lax.dot_general(a, b, (((1,), (1,)), ((), ())), preferred_element_type=F32)


def dot_tn(a, b):
    return lax.dot_general(a, b, (((0,), (0,)), ((), ())), preferred_element_type=F32)


def thirds(x):
    first = x.astype(BF16)
    rest = x - first.astype(F32)
    second = rest.astype(BF16)
    third = (rest - second.astype(F32)).astype(BF16)
    return first, second, third


def halves(x):
    first = x.astype(BF16)
    return first, (x - first.astype(F32)).astype(BF16)


def picked(chooser, values):
    return dot_nn(
        jnp.concatenate([chooser, chooser], axis=1), jnp.concatenate(halves(values), axis=0)
    )


def as_bf16(mask):
    return jnp.where(mask, 1.0, 0.0).astype(BF16)


def as_column(row, size):
    diagonal = iota((size, size), 0) == iota((size, size), 1)
    return jnp.sum(jnp.where(diagonal, row, jnp.zeros((), row.dtype)), axis=1, keepdims=True)


class Sizes:
    def __init__(self, state, links, h_bands, tiers, parts):
        self.slots = state.shape[0]
        self.rows = state.shape[2]
        self.levels = state.shape[3]
        self.band = h_bands.shape[0] - 1
        self.per_slot = links.shape[2]
        self.tiers = tiers
        self.parts = parts
        self.modes = self.per_slot // 2
        self.block_modes = self.modes // parts
        total = self.slots * self.per_slot
        self.cap = total // tiers
        self.row_cap = 2 * ((self.slots * self.block_modes + tiers - 1) // tiers)
        self.lane_tiles = 2 * self.levels // LANES
        self.message = self.cap + self.row_cap * self.lane_tiles
        self.ask = round_up(2 * self.cap, 16)
        self.shift = self.slots.bit_length() - 1
        self.span = round_up(self.slots * self.modes, LANES)
        self.row_pad = round_up(self.slots * self.block_modes, 16)
        self.group = round_up(self.block_modes, 8)


def holders_of(z, links_ref, g):
    neighbour = links_ref[0, g : g + 1, :]
    holder = lax.shift_right_logical(neighbour, z.shift)
    target = lax.bitwise_and(neighbour, z.slots - 1)
    hit = holder == iota((z.tiers, z.per_slot), 0)
    return hit, holder, target


def earlier_table(size):
    return as_bf16(iota((size, size), 0) < iota((size, size), 1))


def rank_of(hit, seen, earlier):
    before = dot_nn(as_bf16(hit), earlier) + seen
    return jnp.sum(jnp.where(hit, before, 0.0), axis=0, keepdims=True).astype(jnp.int32)


def ask_kernel(z, links_ref, out_ref):
    earlier = earlier_table(z.per_slot)
    ones = jnp.ones((z.per_slot, z.per_slot), BF16)
    seen = jnp.zeros((z.tiers, z.per_slot), F32)
    table = jnp.zeros((z.tiers, z.ask), F32)
    field = iota((z.ask, z.per_slot), 0)
    for g in range(z.slots):
        hit, _, target = holders_of(z, links_ref, g)
        mode = links_ref[1, g : g + 1, :]
        rank = rank_of(hit, seen, earlier)
        value = jnp.where(lax.bitwise_and(field, 1) == 0, target, mode)
        value = jnp.where(lax.shift_right_logical(field, 1) == rank, value, 0)
        chosen = as_bf16(hit)
        table = table + dot_nt(chosen, value.astype(F32).astype(BF16))
        seen = seen + dot_nn(chosen, ones)
    out_ref[...] = table.astype(jnp.int32)


def table_kernel(
    z, state_ref, slope_ref, sites_ref, counts_ref, low_ref, high_ref, col_ref, row_ref, mid_ref,
    base_ref, rows_scr, site_scr,
):
    own = counts_ref[lax.axis_index("tier")]
    part = lax.axis_index("sys")
    lane = iota((1, z.levels), 1)
    used = z.slots * z.modes
    for third in range(3):
        if z.span > used:
            col_ref[third * z.span + used : (third + 1) * z.span, :] = jnp.zeros(
                (z.span - used, 2 * z.rows), BF16
            )
    for k in range(z.modes):
        site_scr[k : k + 1, :] = jnp.where(lane == sites_ref[k], 1.0, 0.0)
    at_site = site_scr[: z.modes, :].astype(BF16)
    rows_scr[...] = jnp.zeros_like(rows_scr)
    for g in range(z.slots):
        live = jnp.where(g < own, 1.0, 0.0)
        base_ref[g] = live * (state_ref[g] + (step_size / 6.0) * slope_ref[g])
        mid = state_ref[g] + (0.5 * step_size) * slope_ref[g]
        mid_ref[g] = mid
        for third, values in enumerate(thirds(mid)):
            at = third * z.span + g * z.modes
            col_ref[at : at + z.modes, :] = dot_nt(at_site, values).astype(BF16)
        for c in range(2):
            start = c * z.rows
            low_ref[g, c] = mid_ref[g, start : start + z.band, :]
            high_ref[g, c] = mid_ref[g, start + z.rows - z.band : start + z.rows, :]
            for k in range(z.block_modes):
                local = sites_ref[part * z.block_modes + k] - part * z.rows
                at = g * z.block_modes + k
                rows_scr[at : at + 1, c * z.levels : (c + 1) * z.levels] = mid_ref[
                    g, pl.ds(start + local, 1), :
                ]
    for third, values in enumerate(thirds(rows_scr[...])):
        row_ref[third * z.row_pad : (third + 1) * z.row_pad, :] = values


def answer_kernel(z, ask_ref, col_ref, row_ref, out_ref):
    part = lax.axis_index("sys")
    low = part * z.block_modes
    asked = ask_ref[...]
    columns = []
    row_at = [jnp.full((z.tiers, 1), -1, jnp.int32) for _ in range(z.row_cap)]
    used = jnp.zeros((z.tiers, 1), jnp.int32)
    lanes = iota((z.tiers, z.span), 1)
    for p in range(z.cap):
        target = asked[:, 2 * p : 2 * p + 1]
        mode = asked[:, 2 * p + 1 : 2 * p + 2]
        columns.append(as_bf16(target * z.modes + mode == lanes))
        inside = jnp.logical_and(mode >= low, mode < low + z.block_modes)
        where_row = target * z.block_modes + (mode - low)
        for j in range(z.row_cap):
            take = jnp.logical_and(inside, used == j)
            row_at[j] = jnp.where(take, where_row, row_at[j])
        used = used + jnp.where(inside, 1, 0)
    lanes = iota((z.tiers, 3 * z.row_pad), 1)
    for third in (2, 1):
        lanes = jnp.where(lanes >= third * z.row_pad, lanes - third * z.row_pad, lanes)
    chosen = jnp.concatenate([as_bf16(at == lanes) for at in row_at], axis=0)
    found = dot_nn(chosen, row_ref[...])
    for j in range(z.row_cap):
        for t in range(z.lane_tiles):
            at = z.cap + j * z.lane_tiles + t
            out_ref[pl.ds(at, z.tiers, stride=z.message), :] = found[
                j * z.tiers : (j + 1) * z.tiers, t * LANES : (t + 1) * LANES
            ]
    chosen = jnp.concatenate(columns, axis=0)
    found = dot_nn(jnp.concatenate([chosen] * 3, axis=1), col_ref[...])
    for p in range(z.cap):
        out_ref[pl.ds(p, z.tiers, stride=z.message), :] = found[p * z.tiers : (p + 1) * z.tiers, :]


def choose_kernel(
    z, links_ref, counts_ref, coef_ref, rate_ref, own_ref, sites_ref,
    col_ref, row_ref, col_coef_ref, row_coef_ref, damp_ref, at_ref, site_scr,
):
    part = lax.axis_index("sys")
    tier = lax.axis_index("tier")
    lane = iota((1, z.levels), 1)
    for k in range(z.modes):
        site_scr[k : k + 1, :] = jnp.where(lane == sites_ref[k], 1.0, 0.0)
    at_ref[...] = site_scr[: z.modes, :].astype(BF16)
    low = part * z.block_modes
    earlier = earlier_table(z.per_slot)
    ones = jnp.ones((z.per_slot, z.per_slot), BF16)
    seen = jnp.zeros((z.tiers, z.per_slot), F32)
    seen_rows = jnp.zeros((z.tiers, z.per_slot), F32)
    counts = as_column(counts_ref[...], z.tiers)
    rate = as_column(rate_ref[...], z.modes)
    coefs = [as_column(coef_ref[c : c + 1, :], z.modes) for c in range(2)]
    total = z.slots * z.modes
    for g in range(z.slots):
        hit, holder, target = holders_of(z, links_ref, g)
        mode = links_ref[1, g : g + 1, :]
        kind = links_ref[2, g : g + 1, :]
        level = links_ref[3, g : g + 1, :]
        rank = rank_of(hit, seen, earlier)
        seen = seen + dot_nn(as_bf16(hit), ones)
        inside = jnp.logical_and(mode >= low, mode < low + z.block_modes)
        hit_rows = jnp.logical_and(hit, inside)
        row_rank = rank_of(hit_rows, seen_rows, earlier)
        seen_rows = seen_rows + dot_nn(as_bf16(hit_rows), ones)
        live = target < jnp.sum(jnp.where(hit, counts, 0), axis=0, keepdims=True)
        live = jnp.logical_and(live, own_ref[tier] > g)
        scale = jnp.where(kind == 1, level, 1)
        here = as_bf16(iota((z.cap * z.tiers, z.per_slot), 0) == rank * z.tiers + holder)
        here_row = as_bf16(
            iota((z.row_cap * z.tiers, z.per_slot), 0) == row_rank * z.tiers + holder
        )
        modes = iota((z.modes, z.per_slot), 0)
        group = iota((z.group, z.per_slot), 0)
        for way in range(2):
            wanted = jnp.logical_and(kind == way, live)
            chosen = jnp.where(jnp.logical_and(modes == mode, wanted), scale, 0)
            at = way * total + g * z.modes
            col_ref[at : at + z.modes, :] = dot_nt(
                chosen.astype(F32).astype(BF16), here
            ).astype(BF16)
            own = jnp.logical_and(group + low == mode, jnp.logical_and(inside, wanted))
            at = (way * z.slots + g) * z.group
            row_ref[at : at + z.group, :] = dot_nt(
                jnp.where(own, scale, 0).astype(F32).astype(BF16), here_row
            )
        falling = jnp.where(jnp.logical_and(modes == mode, kind == 1), level, 0).astype(F32)
        amount = jnp.sum(falling, axis=1, keepdims=True) * rate
        damp_ref[g] = jnp.broadcast_to(jnp.sum(amount, axis=0, keepdims=True), (8, LANES))
    for c in range(2):
        col_coef_ref[c] = jnp.broadcast_to(coefs[c], (z.modes, LANES))
        mine = jnp.where(
            iota((z.group, z.modes), 0) + low == iota((z.group, z.modes), 1),
            coef_ref[c : c + 1, :],
            0.0,
        )
        mine = jnp.where(iota((z.group, z.modes), 0) < z.block_modes, mine, 0.0)
        row_coef_ref[c] = jnp.broadcast_to(
            jnp.sum(mine, axis=1, keepdims=True), (z.group, LANES)
        )


def band_kernel(
    z, mid_ref, low_ref, high_ref, bands_ref, damp_ref, counts_ref, out_ref, wide, spread,
    across_ref, mid_scr,
):
    part = lax.axis_index("sys")
    own = counts_ref[lax.axis_index("tier")]
    taps = 2 * z.band + 1
    across_ref[...] = jnp.zeros_like(across_ref)
    lane = iota((1, z.levels), 1)
    for t in range(taps):
        offset = t - z.band
        row = bands_ref[abs(offset) : abs(offset) + 1, :]
        if offset < 0:
            row = jnp.where(lane >= -offset, pltpu.roll(row, -offset, 1), 0.0)
        elif offset > 0:
            row = jnp.where(lane < z.levels - offset, row, 0.0)
        across_ref[t : t + 1, :] = row
    here = as_bf16(
        iota((z.rows, z.levels), 0) + part * z.rows == iota((z.rows, z.levels), 1)
    )
    down = jnp.zeros((z.rows, across_ref.shape[0]), F32)
    for values in thirds(across_ref[...]):
        down = down + dot_nt(here, values)
    for t in range(taps):
        spread[t] = jnp.broadcast_to(down[:, t : t + 1], (z.rows, LANES))
    tiles = z.levels // LANES
    mid_scr[...] = mid_ref[...]
    for g in range(z.slots):
        live = jnp.where(g < own, 1.0, 0.0)
        damp = damp_ref[g, 0:1, 0:1]
        fields = [mid_scr[g, c * z.rows : (c + 1) * z.rows, :] for c in range(2)]
        for c in range(2):
            field = fields[c]
            wide[0 : z.band, :] = low_ref[g, c]
            wide[z.band : z.band + z.rows, :] = field
            wide[z.band + z.rows :, :] = high_ref[g, c]
            summed = across_ref[z.band : z.band + 1, :] * field
            for t in range(taps):
                if t != z.band:
                    moved = pltpu.roll(field, (z.band - t) % z.levels, 1)
                    summed = summed + across_ref[t : t + 1, :] * moved
            sides = []
            for q in range(tiles):
                lanes = slice(q * LANES, (q + 1) * LANES)
                total = spread[0] * wide[0 : z.rows, lanes]
                for t in range(1, taps):
                    total = total + spread[t] * wide[t : t + z.rows, lanes]
                sides.append(total)
            commuted = jnp.concatenate(sides, axis=1) - summed
            other = 1 - c
            sign = 1.0 if c == 1 else -1.0
            out_ref[g, other * z.rows : (other + 1) * z.rows, :] = (
                live * (sign * commuted - damp * fields[other])
            )


def apply_kernel(
    z, got_ref, col_ref, row_ref, col_coef_ref, row_coef_ref, deriv_ref, base_ref,
    at_ref, sites_ref, next_ref, sum_ref, next_scr, sum_scr, sem,
):
    part = lax.axis_index("sys")
    at_site = jnp.concatenate([at_ref[...]] * 2, axis=0)
    total = z.slots * z.modes
    pieces = jnp.concatenate(
        [
            jnp.concatenate(
                [
                    got_ref[pl.ds(z.cap + j * z.lane_tiles + t, z.tiers, stride=z.message), :]
                    for t in range(z.lane_tiles)
                ],
                axis=1,
            )
            for j in range(z.row_cap)
        ],
        axis=0,
    )
    found = picked(row_ref[...].astype(BF16), pieces)
    half = z.slots * z.group
    up, down = found[:half], found[half:]
    real = jnp.concatenate([row_coef_ref[0, :, 0:1]] * z.slots, axis=0)
    imag = jnp.concatenate([row_coef_ref[1, :, 0:1]] * z.slots, axis=0)
    turned = up + real * down
    straight = imag * down
    real_rows = straight[:, : z.levels] + turned[:, z.levels :]
    imag_rows = straight[:, z.levels :] - turned[:, : z.levels]
    target = jnp.full((2 * z.group, 2 * z.rows), -1, jnp.int32)
    line = iota((2 * z.group, 2 * z.rows), 0)
    for k in range(z.block_modes):
        local = sites_ref[part * z.block_modes + k] - part * z.rows
        for c in range(2):
            target = jnp.where(line == c * z.group + k, c * z.rows + local, target)
    at_row = as_bf16(iota((2 * z.group, 2 * z.rows), 1) == target)
    pieces = jnp.concatenate(
        [got_ref[pl.ds(p, z.tiers, stride=z.message), :] for p in range(z.cap)], axis=0
    )
    found = picked(col_ref[...], pieces)
    sign = jnp.where(iota((1, 2 * z.rows), 1) < z.rows, -1.0, 1.0)
    for g in range(z.slots):
        up = found[g * z.modes : (g + 1) * z.modes]
        down = found[total + g * z.modes : total + (g + 1) * z.modes]
        cols = col_coef_ref[1] * down + sign * pltpu.roll(up + col_coef_ref[0] * down, z.rows, 1)
        mine = slice(g * z.group, (g + 1) * z.group)
        own = halves(jnp.concatenate([real_rows[mine], imag_rows[mine]], axis=0))
        slope_next = deriv_ref[g] + dot_tn(
            jnp.concatenate([*halves(cols), at_row, at_row], axis=0),
            jnp.concatenate([at_site, *own], axis=0),
        )
        next_scr[g] = slope_next
        pltpu.make_async_copy(next_scr.at[g], next_ref.at[g], sem.at[0, g]).start()
        sum_scr[g] = base_ref[g] + (step_size / 3.0) * slope_next
        pltpu.make_async_copy(sum_scr.at[g], sum_ref.at[g], sem.at[1, g]).start(priority=1)
    for g in range(z.slots):
        pltpu.make_async_copy(next_scr.at[g], next_ref.at[g], sem.at[0, g]).wait()
        pltpu.make_async_copy(sum_scr.at[g], sum_ref.at[g], sem.at[1, g]).wait()


def call(kernel, z, name, args, in_specs, outs, scratch=(), out_specs=None, micros=1, aliases=()):
    return pl.pallas_call(
        functools.partial(kernel, z),
        out_shape=outs,
        in_specs=in_specs,
        out_specs=[VMEM] * len(outs) if out_specs is None else out_specs,
        scratch_shapes=list(scratch),
        name=name,
        input_output_aliases=dict(aliases),
        compiler_params=pltpu.CompilerParams(vmem_limit_bytes=int(vmem_limits.get(name, 16) * mib)),
        cost_estimate=pl.CostEstimate(
            flops=int(micros * 1e6), bytes_accessed=int(micros * 1e5), transcendentals=0
        ),
    )(*args)


def neighbours(low_edge, high_edge):
    count = lax.axis_size("sys")
    forward = [(i, i + 1) for i in range(count - 1)]
    backward = [(target, source) for source, target in forward]
    return lax.ppermute(high_edge, "sys", forward), lax.ppermute(low_edge, "sys", backward)


def shards(state, slope, counts, links, mode_site, mode_coef, mode_rate, h_bands):
    z = Sizes(state, links, h_bands, lax.axis_size("tier"), lax.axis_size("sys"))
    shape = jax.ShapeDtypeStruct
    flat = (z.slots, 2 * z.rows, z.levels)
    state_flat = state.reshape(flat)
    slope_flat = slope.reshape(flat)
    (ask,) = call(
        ask_kernel, z, "ask", (links,), [VMEM], [shape((z.tiers, z.ask), jnp.int32)]
    )
    asked = lax.all_to_all(
        ask.reshape(z.tiers, 1, z.ask), "tier", split_axis=0, concat_axis=0, tiled=True
    ).reshape(z.tiers, z.ask)
    edge = (z.slots, 2, z.band, z.levels)
    low_edge, high_edge, col_table, row_table, mid, base = call(
        table_kernel,
        z,
        "tables",
        (state_flat, slope_flat, mode_site, counts),
        [VMEM, VMEM, SMEM, SMEM],
        [
            shape(edge, F32),
            shape(edge, F32),
            shape((3 * z.span, 2 * z.rows), BF16),
            shape((3 * z.row_pad, 2 * z.levels), BF16),
            shape(flat, F32),
            shape(flat, F32),
        ],
        [
            pltpu.VMEM((z.row_pad, 2 * z.levels), F32),
            pltpu.VMEM((round_up(z.modes, 16), z.levels), F32),
        ],
        micros=3,
    )
    (answer,) = call(
        answer_kernel,
        z,
        "answer",
        (asked, col_table, row_table),
        [VMEM] * 3,
        [shape((z.tiers * z.message, LANES), F32)],
    )
    got = lax.all_to_all(
        answer.reshape(z.tiers, 1, z.message * LANES),
        "tier",
        split_axis=0,
        concat_axis=0,
        tiled=True,
    ).reshape(z.tiers * z.message, LANES)
    low_edge, high_edge, answer_kept = lax.optimization_barrier((low_edge, high_edge, answer))
    above, below = neighbours(low_edge, high_edge)
    col_choice, row_choice, col_coef, row_coef, damp, at_site = call(
        choose_kernel,
        z,
        "choose",
        (links, counts[None], mode_coef, mode_rate[None], counts, mode_site),
        [VMEM] * 4 + [SMEM] * 2,
        [
            shape((2 * z.slots * z.modes, z.cap * z.tiers), BF16),
            shape((2 * z.slots * z.group, z.row_cap * z.tiers), F32),
            shape((2, z.modes, LANES), F32),
            shape((2, z.group, LANES), F32),
            shape((z.slots, 8, LANES), F32),
            shape((z.modes, z.levels), BF16),
        ],
        [pltpu.VMEM((round_up(z.modes, 16), z.levels), F32)],
        micros=2,
    )
    taps = round_up(2 * z.band + 1, 16)
    (deriv,) = call(
        band_kernel,
        z,
        "band",
        (mid, above, below, h_bands, damp, counts),
        [VMEM] * 5 + [SMEM],
        [shape(flat, F32)],
        [
            pltpu.VMEM((z.rows + 2 * z.band, z.levels), F32),
            pltpu.VMEM((2 * z.band + 1, z.rows, LANES), F32),
            pltpu.VMEM((taps, z.levels), F32),
            pltpu.VMEM(flat, F32),
        ],
        aliases=((0, 0),),
        micros=5,
    )
    slope_next, partial_sum = call(
        apply_kernel,
        z,
        "apply",
        (
            got, col_choice, row_choice, col_coef, row_coef, deriv, base, at_site, mode_site,
        ),
        [VMEM] * 8 + [SMEM],
        [shape(flat, F32), shape(flat, F32)],
        [
            pltpu.VMEM(flat, F32),
            pltpu.VMEM(flat, F32),
            pltpu.SemaphoreType.DMA((2, z.slots)),
        ],
        out_specs=[HBM, HBM],
        micros=4,
    )
    return slope_next.reshape(state.shape), partial_sum.reshape(state.shape)


def solution(mesh):
    in_specs = (
        P("tier", None, "sys", None),
        P("tier", None, "sys", None),
        P(),
        P(None, "tier", None),
        P(),
        P(),
        P(),
        P(),
    )
    out_specs = (P("tier", None, "sys", None), P("tier", None, "sys", None))
    return jax.shard_map(shards, mesh=mesh, in_specs=in_specs, out_specs=out_specs, check_vma=False)
```
